32 devices in a mesh: dp: 4 (over y, x), seq: 4 (over z), tensor: 2 (over core).
Axes of the slice: x: 2, y: 2, z: 4, core: 2. Of those that a mesh axis runs over, the one named last changes fastest.
Arguments:
- hidden: bfloat16 [4, 1024, 2048], P('dp', 'seq'), may hold values from -6 to 6
- lengths: int32 [4], P('dp'), may hold values from 256 to 1024, as said below
- pre_gain: float32 [2, 2048], replicated, may hold values from 0.5 to 1.5
- w_zx: bfloat16 [2, 2048, 2, 4096], P(None, ('dp', 'seq'), None, 'tensor'), may hold values from -0.125 to 0.125
- w_bc: bfloat16 [2, 2048, 256], P(None, ('dp', 'seq'), 'tensor'), may hold values from -0.125 to 0.125
- w_dt: bfloat16 [2, 2048, 64], P(None, ('dp', 'seq'), 'tensor'), may hold values from -0.125 to 0.125
- conv_x: float32 [2, 5, 4096], P(None, None, 'tensor'), may hold values from -0.5 to 0.5
- conv_bc: float32 [2, 5, 256], P(None, None, 'tensor'), may hold values from -0.5 to 0.5
- head_params: float32 [2, 3, 64], P(None, None, 'tensor'), may hold values from -9 to 2, as said below
- norm_gain: float32 [2, 4096], P(None, 'tensor'), may hold values from 0.5 to 1.5
- w_out: bfloat16 [2, 4096, 2048], P(None, 'tensor', ('dp', 'seq')), may hold values from -0.09375 to 0.09375
- cotangent: bfloat16 [4, 1024, 2048], P('dp', 'seq'), may hold values from -6 to 6
Outputs:
- out: bfloat16 [4, 1024, 2048], P('dp', 'seq')
- d_hidden: float32 [4, 1024, 2048], P('dp', 'seq')
- d_pre_gain: float32 [2, 2048], replicated
- d_w_zx: float32 [2, 2048, 2, 4096], P(None, ('dp', 'seq'), None, 'tensor')
- d_w_bc: float32 [2, 2048, 256], P(None, ('dp', 'seq'), 'tensor')
- d_w_dt: float32 [2, 2048, 64], P(None, ('dp', 'seq'), 'tensor')
- d_conv_x: float32 [2, 5, 4096], P(None, None, 'tensor')
- d_conv_bc: float32 [2, 5, 256], P(None, None, 'tensor')
- d_head_params: float32 [2, 3, 64], P(None, None, 'tensor')
- d_norm_gain: float32 [2, 4096], P(None, 'tensor')
- d_w_out: float32 [2, 4096, 2048], P(None, 'tensor', ('dp', 'seq'))
The draws below stay inside these ranges and needn't reach their ends.
Inputs may be any that keep to these rules, and one draw needn't show every extreme that they name: `lengths`: each sequence's real tokens come first; at least 256 of them, and one sequence has exactly 1024. `head_params`: row 0 the log of a head's decay rate, row 1 its step bias, row 2 its skip weight.
All inputs are finite; a program needn't handle non-finite values.
Results may differ from the reference program's by a relative error of at most 0.022.
Values may be sent and summed in bfloat16 or wider, within the bound.
A program may use at most 256 MiB of HBM per device.

```python
import jax
import jax.numpy as jnp
from jax import lax

D = 2048
DI = 4096
H = 64
P_SIZE = 64
N = 128
K = 4
Q = 256
L = 2
LEN = 1024
SEQS = 4


def draw_lengths(key, part):
    values = jax.random.randint(key, (SEQS,), LEN // 4, LEN + 1)
    longest = jax.random.randint(jax.random.fold_in(key, 7), (), 0, SEQS)
    return jnp.where(jnp.arange(SEQS) == longest, LEN, values).astype(jnp.int32)


def draw_head_params(key, part):
    keys = jax.random.split(key, 3)
    decay_log = jax.random.uniform(keys[0], (L, 1, H), jnp.float32, -4.0, 1.0)
    step_bias = jax.random.uniform(keys[1], (L, 1, H), jnp.float32, -8.0, -2.0)
    skip_weight = jax.random.uniform(keys[2], (L, 1, H), jnp.float32, 0.5, 1.5)
    return jnp.concatenate([decay_log, step_bias, skip_weight], axis=1)


def steps_of(own_key, extent, cuts, least, high):
    level, own = 1.0, jax.random.fold_in(own_key, 6)
    for axis_at, parts in cuts:
        heights = jnp.exp(jax.random.uniform(jax.random.fold_in(own, axis_at), (parts,), jnp.float32, least / len(cuts), high / len(cuts)))
        level = level * jnp.repeat(heights, extent[axis_at] // parts).reshape([-1 if axis == axis_at else 1 for axis in range(len(extent))])
    return level


def gaussian(rng, shape, width, bound, cuts=(), kind=jnp.bfloat16):
    values = jax.random.normal(rng, shape, jnp.float32) * width
    if len(cuts) > 0:
        values = steps_of(rng, shape, cuts, -0.22, 0.18) * values
    return jnp.clip(values, min=-bound, max=bound).astype(kind)


def setup_inputs(seed: int = 0) -> dict:
    arg_keys = jax.random.split(jax.random.key(seed), 13)
    return {
        "hidden": gaussian(arg_keys[0], (SEQS, LEN, D), 1.0, 6.0, ((0, 4), (1, 4))),
        "lengths": draw_lengths(jax.random.fold_in(arg_keys[12], 71), 0),
        "pre_gain": jnp.clip(1.0 + 0.1 * jax.random.normal(arg_keys[2], (L, D), jnp.float32), 0.5, 1.5),
        "w_zx": gaussian(arg_keys[3], (L, D, 2, DI), D ** -0.5, 0.125, ((1, 16), (3, 2))),
        "w_bc": gaussian(arg_keys[4], (L, D, 2 * N), D ** -0.5, 0.125, ((1, 16), (2, 2))),
        "w_dt": gaussian(arg_keys[5], (L, D, H), D ** -0.5, 0.125, ((1, 16), (2, 2))),
        "conv_x": jnp.clip(jax.random.uniform(arg_keys[6], (L, K + 1, DI), jnp.float32, -0.5, 0.5) * steps_of(arg_keys[6], (L, K + 1, DI), ((2, 2),), -0.4, 0.0), -0.5, 0.5),
        "conv_bc": jnp.clip(jax.random.uniform(arg_keys[7], (L, K + 1, 2 * N), jnp.float32, -0.5, 0.5) * steps_of(arg_keys[7], (L, K + 1, 2 * N), ((2, 2),), -0.4, 0.0), -0.5, 0.5),
        "head_params": draw_head_params(jax.random.fold_in(arg_keys[12], 71), 0),
        "norm_gain": jnp.clip(1.0 + 0.1 * jax.random.normal(arg_keys[9], (L, DI), jnp.float32), 0.5, 1.5),
        "w_out": gaussian(arg_keys[10], (L, DI, D), DI ** -0.5, 0.09375, ((1, 2), (2, 16))),
        "cotangent": gaussian(arg_keys[11], (SEQS, LEN, D), 1.0, 6.0, ((0, 4), (1, 4))),
    }


PRECISE = lax.Precision.HIGHEST
EPSILON = 1e-05

@jax.custom_vjp
def low(v):
    return lax.optimization_barrier(v.astype(jnp.bfloat16)).astype(jnp.float32)

@jax.custom_vjp
def low_back(v):
    return v

def low_keep(v):
    return (low(v), None)

def low_pass(kept, grad):
    return (grad,)

def back_keep(v):
    return (v, None)

def back_low(kept, grad):
    return (low(grad),)
low.defvjp(low_keep, low_pass)
low_back.defvjp(back_keep, back_low)

def conv_silu(values, kernel):
    padded = jnp.pad(values, ((0, 0), (K - 1, 0), (0, 0)))
    row_count = values.shape[1]
    running = kernel[K]
    for offset in range(K):
        running = running + kernel[offset] * padded[:, offset:offset + row_count]
    return jax.nn.silu(running)

def state_space(inputs, b_rows, c_rows, step_sizes, decay_rate, skip_weight):
    seq_count = inputs.shape[0]
    blocks = inputs.shape[1] // Q

    def blocked(values):
        return jnp.moveaxis(values.reshape((seq_count, blocks, Q) + values.shape[2:]), 1, 0)
    causal = jnp.arange(Q)[:, None] >= jnp.arange(Q)[None, :]

    @jax.checkpoint
    def advance(carried, pieces):
        inputs_block, b_block, c_block, step_block = pieces
        cumulative = jnp.cumsum(step_block * decay_rate, axis=1)
        heads_cum = jnp.moveaxis(cumulative, 2, 1)
        scores = jnp.einsum('sqn,skn->sqk', c_block, b_block, precision=PRECISE)
        spread = heads_cum[:, :, :, None] - heads_cum[:, :, None, :]
        mixing = jnp.where(causal, jnp.exp(jnp.minimum(spread, 0.0)), 0.0)
        mixing = mixing * scores[:, None] * jnp.moveaxis(step_block, 2, 1)[:, :, None, :]
        within = jnp.einsum('shqk,skhp->sqhp', mixing, inputs_block, precision=PRECISE)
        across = jnp.einsum('sqn,shpn->sqhp', c_block, carried, precision=PRECISE) * jnp.exp(cumulative)[..., None]
        tail_weight = jnp.exp(cumulative[:, -1:] - cumulative) * step_block
        fresh_state = jnp.einsum('sqhp,sqn->shpn', tail_weight[..., None] * inputs_block, b_block, precision=PRECISE)
        carried = jnp.exp(cumulative[:, -1])[..., None, None] * carried + fresh_state
        return (carried, within + across + skip_weight[:, None] * inputs_block)
    initial = jnp.zeros((seq_count, H, P_SIZE, N), jnp.float32)
    unused_state, outputs = lax.scan(advance, initial, (blocked(inputs), blocked(b_rows), blocked(c_rows), blocked(step_sizes)))
    return jnp.moveaxis(outputs, 0, 1).reshape(inputs.shape)

def block(residual, live_mask, gain_pre, w_pairs_zx, w_pair, w_step, kernel_x, kernel_pair, head_rows, gain_norm, w_mix):
    seq_count = residual.shape[0]
    seq_len = residual.shape[1]
    live_col = live_mask[..., None]
    normed = low(residual * lax.rsqrt(lax.optimization_barrier(jnp.mean(residual * residual, axis=-1, keepdims=True)) + EPSILON) * gain_pre)
    gate_raw = low_back(jnp.dot(normed, w_pairs_zx[:, 0], precision=PRECISE))
    inner_low = low(low_back(jnp.dot(normed, w_pairs_zx[:, 1], precision=PRECISE))) * live_col
    pair_raw = low(low_back(jnp.dot(normed, w_pair, precision=PRECISE))) * live_col
    step_raw = low_back(jnp.dot(normed, w_step, precision=PRECISE))
    inputs = low(conv_silu(inner_low, kernel_x)).reshape(seq_count, seq_len, H, P_SIZE)
    pair_rows = low(conv_silu(pair_raw, kernel_pair))
    step_sizes = jax.nn.softplus(step_raw + head_rows[1]) * live_col
    decay_rate = -jnp.exp(head_rows[0])
    outputs = state_space(inputs, pair_rows[..., :N], pair_rows[..., N:], step_sizes, decay_rate, head_rows[2])
    outputs = outputs.reshape(seq_count, seq_len, DI)
    gated_out = outputs * jax.nn.silu(gate_raw)
    mixed_in = low(gated_out * lax.rsqrt(lax.optimization_barrier(jnp.mean(gated_out * gated_out, axis=-1, keepdims=True)) + EPSILON) * gain_norm)
    return residual + low_back(jnp.dot(mixed_in, w_mix, precision=PRECISE))

def reference(hidden, lengths, pre_gain, w_zx, w_bc, w_dt, conv_x, conv_bc, head_params, norm_gain, w_out, cotangent):
    positions = jnp.arange(LEN, dtype=jnp.int32)
    live_mask = (positions[None, :] < lengths[:, None]).astype(jnp.float32)
    params = (pre_gain, w_zx.astype(jnp.float32), w_bc.astype(jnp.float32), w_dt.astype(jnp.float32), conv_x, conv_bc, head_params, norm_gain, w_out.astype(jnp.float32))

    def forward(residual, weights):
        for layer_index in range(L):
            residual = block(residual, live_mask, *[weight[layer_index] for weight in weights])
        return residual
    result, pull_back = jax.vjp(forward, hidden.astype(jnp.float32), params)
    grad_hidden, grads = pull_back(cotangent.astype(jnp.float32))
    return (result.astype(jnp.bfloat16), grad_hidden, grads[0], grads[1], grads[2], grads[3], grads[4], grads[5], grads[6], grads[7], grads[8])
```

```python
import functools

import jax
import jax.numpy as jnp
from jax import lax
from jax.experimental import pallas as pl
from jax.experimental.pallas import tpu as pltpu
from jax.sharding import PartitionSpec as P

DI = 4096
P_SIZE = 64
N = 128
K = 4
Q = 256
L = 2
LANES = 128
EPSILON = 1e-05
F32 = jnp.float32
BF16 = jnp.bfloat16
PRECISE = lax.Precision.HIGHEST


def swap(value, axis, distance):
    size = lax.axis_size(axis)
    return lax.ppermute(value, axis, [(i, i ^ distance) for i in range(size)])


def pick(value, index):
    return lax.dynamic_index_in_dim(value, index, 0, False)


def put(buffer, value, index):
    return lax.dynamic_update_index_in_dim(buffer, value, index, 0)


def gather_axis(value, axis):
    size, place = lax.axis_size(axis), lax.axis_index(axis)
    out = put(jnp.zeros((size,) + value.shape, value.dtype), value, place)
    for distance in range(1, size):
        out = put(out, swap(value, axis, distance), place ^ distance)
    return out


def exchange_axis(values, axis):
    size, place = lax.axis_size(axis), lax.axis_index(axis)
    out = put(jnp.zeros_like(values), pick(values, place), place)
    for distance in range(1, size):
        out = put(out, swap(pick(values, place ^ distance), axis, distance), place ^ distance)
    return out


def scatter_axis(values, axis, kind=BF16):
    size, place = lax.axis_size(axis), lax.axis_index(axis)
    total = pick(values, place).astype(F32)
    for distance in range(1, size):
        sent = pick(values, place ^ distance).astype(kind)
        total = total + swap(sent, axis, distance).astype(F32)
    return total


def sum_axis(value, axis, kind=F32):
    size = lax.axis_size(axis)
    distance = 1
    while distance < size:
        value = value + swap(value.astype(kind), axis, distance).astype(value.dtype)
        distance *= 2
    return value


def gather_rows(own):
    along = gather_axis(own, "seq")
    both = jnp.swapaxes(gather_axis(along, "tensor"), 0, 1)
    return both.reshape((-1,) + own.shape[1:])


def scatter_rows(partial):
    seqs, cores = lax.axis_size("seq"), lax.axis_size("tensor")
    parts = partial.reshape((seqs, cores, -1) + partial.shape[1:])
    halves = scatter_axis(jnp.swapaxes(parts, 0, 1), "tensor")
    return scatter_axis(halves, "seq")


def lane_iota(shape):
    return lax.broadcasted_iota(jnp.int32, shape, len(shape) - 1)


def row_iota(shape):
    return lax.broadcasted_iota(jnp.int32, shape, len(shape) - 2)


def dot(a, b, dims, precision=None):
    return lax.dot_general(
        a, b, (dims, ((), ())), preferred_element_type=F32, precision=precision
    )


NN = ((1,), (0,))
NT = ((1,), (1,))
TN = ((0,), (0,))


def pair_of(columns, j):
    rows = columns.shape[0]
    first = lane_iota((rows, LANES)) < P_SIZE
    return jnp.where(first, columns[:, 2 * j : 2 * j + 1], columns[:, 2 * j + 1 : 2 * j + 2])


def spread(columns, heads):
    return jnp.concatenate([pair_of(columns, j) for j in range(heads // 2)], axis=1)


def split_pair(pair):
    first = lane_iota(pair.shape) < P_SIZE
    zero = jnp.zeros_like(pair)
    return jnp.where(first, pair, zero), jnp.where(first, zero, pair)


def block_steps(raw, head_rows, live):
    steps = jax.nn.softplus(raw + head_rows[1:2]) * live
    rate = -jnp.exp(head_rows[0:1])
    return steps, rate


def sigmoid(v):
    return 1.0 / (1.0 + jnp.exp(-v))


def forward_kernel(
    sizes, length_ref, proj_ref, pairs_ref, conv_ref, head_ref, gain_ref,
    outputs_ref, mixed_ref, inputs_ref, states_ref, square_ref, state, halo,
):
    tokens, inner, heads, step_at = sizes
    head_rows = head_ref[...]
    head_lane = lane_iota((1, LANES)) < heads
    causal = row_iota((Q, Q)) >= lane_iota((Q, Q))
    below = causal.astype(F32)
    state[...] = jnp.zeros_like(state)
    halo[...] = jnp.zeros_like(halo)
    length = length_ref[0]

    def block(k, carry):
        start = pl.multiple_of(k * Q, Q)
        rows = pl.ds(start, Q)
        live = (row_iota((Q, 1)) + start < length).astype(F32)
        raw = (proj_ref[rows, inner : 2 * inner].astype(F32) * live).astype(BF16).astype(F32)
        padded = jnp.concatenate([halo[...], raw], axis=0)
        halo[...] = raw[Q - 8 :]
        pre = conv_ref[K : K + 1, :]
        for tap in range(K):
            pre = pre + conv_ref[tap : tap + 1, :] * padded[5 + tap : 5 + tap + Q]
        inputs = (pre * sigmoid(pre)).astype(BF16)
        inputs_ref[rows, :] = inputs
        steps, rate = block_steps(proj_ref[rows, step_at : step_at + LANES], head_rows, live)
        decay = jnp.where(head_lane, steps * rate, 0.0)
        cum = dot(below, decay, NN, PRECISE)
        cum_t = cum.T
        b_rows = pairs_ref[rows, :N]
        c_rows = pairs_ref[rows, N:]
        scores = jnp.where(causal, dot(c_rows, b_rows, NT), 0.0)
        before = state[...]
        states_ref[k] = before
        inputs_f = inputs.astype(F32)
        scaled = inputs_f * spread(steps, heads)
        scaled_low = scaled.astype(BF16)
        across = dot(c_rows, before.astype(BF16), NT) * spread(jnp.exp(cum), heads)
        last = cum[Q - 1 : Q]
        tail = jnp.exp(last - cum)
        square = jnp.zeros((8, Q), F32)
        for j in range(heads // 2):
            cols = slice(j * LANES, (j + 1) * LANES)
            mixing = []
            for h in (2 * j, 2 * j + 1):
                gap = jnp.minimum(cum[:, h : h + 1] - cum_t[h : h + 1, :], 0.0)
                mixing.append((jnp.exp(gap) * scores).astype(BF16))
            both = jnp.concatenate(mixing, axis=1)
            stacked = jnp.concatenate(split_pair(scaled_low[:, cols]), axis=0)
            out = dot(both, stacked, NN) + across[:, cols]
            out = out + pair_of(head_rows[2:3], j) * inputs_f[:, cols]
            outputs_ref[rows, cols] = out
            gate = proj_ref[rows, cols]
            gated = out * gate * sigmoid(gate)
            mixed_ref[rows, cols] = (gated * gain_ref[:, cols]).astype(BF16)
            square = square + dot(jnp.ones((8, LANES), F32), gated * gated, NT, PRECISE)
        for part in range(Q // LANES):
            square_ref[pl.ds(k * (Q // LANES) + part, 1), :] = square[
                0:1, part * LANES : (part + 1) * LANES
            ]
        fresh = dot((scaled * spread(tail, heads)).astype(BF16), b_rows, TN)
        for h in range(heads):
            own = slice(h * P_SIZE, (h + 1) * P_SIZE)
            state[own, :] = jnp.exp(last[:, h : h + 1]) * before[own] + fresh[own]
        return carry

    lax.fori_loop(0, tokens // Q, block, 0)


def backward_kernel(
    sizes, length_ref, proj_ref, pairs_ref, conv_ref, head_ref, gain_ref, inputs_ref,
    outputs_ref, states_ref, mixgrad_ref, scale_ref, coef_ref,
    mixed_ref, slab_ref, bc_ref, conv_grad_ref, head_grad_ref, small_ref, state, halo,
    scratch_a, scratch_b, scratch_c,
):
    tokens, inner, heads, step_at = sizes
    head_rows = head_ref[...]
    head_lane = lane_iota((1, LANES)) < heads
    causal = row_iota((Q, Q)) >= lane_iota((Q, Q))
    below = causal.astype(F32)
    onehot = (row_iota((inner, LANES)) // P_SIZE == lane_iota((inner, LANES))).astype(F32)
    state[...] = jnp.zeros_like(state)
    halo[...] = jnp.zeros_like(halo)
    conv_grad_ref[...] = jnp.zeros_like(conv_grad_ref)
    head_grad_ref[...] = jnp.zeros_like(head_grad_ref)
    small_ref[...] = jnp.zeros_like(small_ref)
    length = length_ref[0]
    blocks = tokens // Q

    def block(turn, carry):
        k = blocks - 1 - turn
        start = pl.multiple_of(k * Q, Q)
        rows = pl.ds(start, Q)
        live = (row_iota((Q, 1)) + start < length).astype(F32)
        steps, rate = block_steps(proj_ref[rows, step_at : step_at + LANES], head_rows, live)
        decay = jnp.where(head_lane, steps * rate, 0.0)
        cum = dot(below, decay, NN, PRECISE)
        cum_t = cum.T
        last = cum[Q - 1 : Q]
        grow = jnp.exp(cum)
        tail = jnp.exp(last - cum)
        b_rows = pairs_ref[rows, :N]
        c_rows = pairs_ref[rows, N:]
        scores = jnp.where(causal, dot(c_rows, b_rows, NT), 0.0)
        before = states_ref[k]
        before_low = before.astype(BF16)
        after = state[...]
        after_low = after.astype(BF16)
        scale = scale_ref[rows, :]
        coef = coef_ref[rows, :]
        spread_b = dot(b_rows, after_low, NT)
        pair_sum = jnp.zeros((Q, Q), F32)
        for j in range(heads // 2):
            cols = slice(j * LANES, (j + 1) * LANES)
            steps_j, grow_j, tail_j = pair_of(steps, j), pair_of(grow, j), pair_of(tail, j)
            skip_j = pair_of(head_rows[2:3], j)
            gate = proj_ref[rows, cols]
            sig = sigmoid(gate)
            silu = gate * sig
            out = outputs_ref[rows, cols]
            gated = out * silu
            mixgrad = mixgrad_ref[rows, cols]
            gain = gain_ref[:, cols]
            normal = gated * scale
            small_ref[0:1, cols] += jnp.sum(mixgrad * normal, axis=0, keepdims=True)
            mixed_ref[rows, cols] = (normal * gain).astype(BF16)
            d_gated = scale * (mixgrad * gain) - gated * coef
            d_out = d_gated * silu
            slab_ref[rows, cols] = (
                d_gated * out * sig * (1.0 + gate * (1.0 - sig))
            ).astype(BF16)
            d_low = d_out.astype(BF16)
            inputs = inputs_ref[rows, cols].astype(F32)
            small_ref[1:2, cols] += jnp.sum(d_out * inputs, axis=0, keepdims=True)
            scaled = inputs * steps_j
            scaled_low = scaled.astype(BF16)
            d_halves = split_pair(d_low)
            mixing = []
            for at, h in enumerate((2 * j, 2 * j + 1)):
                gap = jnp.minimum(cum[:, h : h + 1] - cum_t[h : h + 1, :], 0.0)
                fade = jnp.exp(gap)
                mixing.append((fade * scores).astype(BF16))
                pair_sum = pair_sum + fade * dot(d_halves[at], scaled_low, NT)
            y_tail = spread_b[:, cols] * tail_j
            y = dot(jnp.concatenate(mixing, axis=0), jnp.concatenate(d_halves, axis=0), TN)
            y = y + y_tail
            scaled_f = scaled_low.astype(F32)
            scratch_a[:, cols] = inputs * y
            scratch_b[:, cols] = d_low.astype(F32) * (out - skip_j * inputs) - scaled_f * y
            small_ref[2:3, cols] = jnp.sum(scaled_f * y_tail, axis=0, keepdims=True)
            scratch_c[:, cols] = steps_j * y + skip_j * d_out
            mixed_low = (d_out * grow_j).astype(BF16)
            slab_ref[rows, inner + j * LANES : inner + (j + 1) * LANES] = mixed_low
        grown = slab_ref[rows, inner : 2 * inner]
        pair_low = jnp.where(causal, pair_sum, 0.0).astype(BF16)
        tailed = (inputs_ref[rows, :].astype(F32) * spread(steps * tail, heads)).astype(BF16)
        bc_ref[rows, :N] = dot(pair_low, c_rows, TN) + dot(tailed, after_low, NN)
        bc_ref[rows, N:] = dot(pair_low, b_rows, NN) + dot(grown, before_low, NN)
        kept = dot(jnp.ones((8, N), F32), after_low.astype(F32) * before, NT, PRECISE)
        ends = dot(kept, onehot, NN, PRECISE)[0:1] * jnp.exp(last)
        ends = ends + dot(
            jnp.broadcast_to(small_ref[2:3, :], (8, inner)), onehot, NN, PRECISE
        )[0:1]
        d_decay = dot(below, dot(scratch_b[...], onehot, NN, PRECISE), TN, PRECISE) + ends
        d_steps = dot(scratch_a[...], onehot, NN, PRECISE) + rate * d_decay
        d_soft = d_steps * live * sigmoid(
            proj_ref[rows, step_at : step_at + LANES] + head_rows[1:2]
        )
        d_soft = jnp.where(head_lane, d_soft, 0.0)
        slab_ref[rows, step_at : step_at + LANES] = d_soft.astype(BF16)
        head_grad_ref[0:1, :] += rate * jnp.sum(
            jnp.where(head_lane, steps * d_decay, 0.0), axis=0, keepdims=True
        )
        head_grad_ref[1:2, :] += jnp.sum(d_soft, axis=0, keepdims=True)
        gathered = dot(grown, c_rows, TN)
        for h in range(heads):
            own = slice(h * P_SIZE, (h + 1) * P_SIZE)
            state[own, :] = jnp.exp(last[:, h : h + 1]) * after[own] + gathered[own]
        raw = (proj_ref[rows, inner : 2 * inner] * live).astype(BF16).astype(F32)
        ahead = pl.ds(pl.multiple_of(jnp.maximum(start - 8, 0), 8), 8)
        earlier = row_iota((8, 1)) + start - 8
        ahead_live = jnp.logical_and(earlier >= 0, earlier < length).astype(F32)
        first = (proj_ref[ahead, inner : 2 * inner] * ahead_live).astype(BF16).astype(F32)
        padded = jnp.concatenate([first, raw], axis=0)
        pre = conv_ref[K : K + 1, :]
        for tap in range(K):
            pre = pre + conv_ref[tap : tap + 1, :] * padded[5 + tap : 5 + tap + Q]
        sig = sigmoid(pre)
        d_pre = scratch_c[...] * sig * (1.0 + pre * (1.0 - sig))
        after_pre = jnp.concatenate([d_pre, halo[...]], axis=0)
        halo[...] = d_pre[0:8]
        d_raw = jnp.zeros((Q, inner), F32)
        for tap in range(K):
            conv_grad_ref[tap : tap + 1, :] += jnp.sum(
                d_pre * padded[5 + tap : 5 + tap + Q], axis=0, keepdims=True
            )
            d_raw = d_raw + conv_ref[tap : tap + 1, :] * after_pre[3 - tap : 3 - tap + Q]
        conv_grad_ref[K : K + 1, :] += jnp.sum(d_pre, axis=0, keepdims=True)
        slab_ref[rows, inner : 2 * inner] = (d_raw * live).astype(BF16)
        return carry

    lax.fori_loop(0, blocks, block, 0)


VMEM_SPEC = pl.BlockSpec(memory_space=pltpu.VMEM)
SMEM_SPEC = pl.BlockSpec(memory_space=pltpu.SMEM)
PARAMS = pltpu.CompilerParams(vmem_limit_bytes=56 * 1024 * 1024)


def run_forward(sizes, lengths, proj, pairs, conv, heads_in, gain):
    tokens, inner, heads, step_at = sizes
    shapes = (
        jax.ShapeDtypeStruct((tokens, inner), F32),
        jax.ShapeDtypeStruct((tokens, inner), BF16),
        jax.ShapeDtypeStruct((tokens, inner), BF16),
        jax.ShapeDtypeStruct((tokens // Q, inner, N), F32),
        jax.ShapeDtypeStruct((tokens // LANES, LANES), F32),
    )
    return pl.pallas_call(
        functools.partial(forward_kernel, sizes),
        out_shape=shapes,
        in_specs=[SMEM_SPEC] + [VMEM_SPEC] * 5,
        out_specs=[VMEM_SPEC] * 5,
        scratch_shapes=[pltpu.VMEM((inner, N), F32), pltpu.VMEM((8, inner), F32)],
        compiler_params=PARAMS,
        cost_estimate=pl.CostEstimate(flops=8 * 10**9, bytes_accessed=16 * 10**6, transcendentals=4 * 10**6),
        name="scan_forward",
    )(lengths, proj, pairs, conv, heads_in, gain)


def run_backward(sizes, lengths, proj, pairs, conv, heads_in, gain, inputs, outputs, states, mixgrad, scale, coef):
    tokens, inner, heads, step_at = sizes
    width = proj.shape[1]
    shapes = (
        jax.ShapeDtypeStruct((tokens, inner), BF16),
        jax.ShapeDtypeStruct((tokens, width), BF16),
        jax.ShapeDtypeStruct((tokens, 2 * N), F32),
        jax.ShapeDtypeStruct((8, inner), F32),
        jax.ShapeDtypeStruct((8, LANES), F32),
        jax.ShapeDtypeStruct((8, inner), F32),
    )
    return pl.pallas_call(
        functools.partial(backward_kernel, sizes),
        out_shape=shapes,
        in_specs=[SMEM_SPEC] + [VMEM_SPEC] * 11,
        out_specs=[VMEM_SPEC] * 6,
        scratch_shapes=[
            pltpu.VMEM((inner, N), F32),
            pltpu.VMEM((8, inner), F32),
            pltpu.VMEM((Q, inner), F32),
            pltpu.VMEM((Q, inner), F32),
            pltpu.VMEM((Q, inner), F32),
        ],
        compiler_params=PARAMS,
        cost_estimate=pl.CostEstimate(flops=20 * 10**9, bytes_accessed=24 * 10**6, transcendentals=6 * 10**6),
        name="scan_backward",
    )(lengths, proj, pairs, conv, heads_in, gain, inputs, outputs, states, mixgrad, scale, coef)


def conv_silu(padded, kernel):
    row_count = padded.shape[0] - K + 1
    running = kernel[K]
    for offset in range(K):
        running = running + kernel[offset] * padded[offset : offset + row_count]
    return jax.nn.silu(running)


def prenorm(residual, gain_pre):
    return (
        residual
        * lax.rsqrt(jnp.mean(residual * residual, axis=-1, keepdims=True) + EPSILON)
        * gain_pre
    )


def pad_to(value, rows, columns):
    return jnp.pad(value, ((0, rows - value.shape[0]), (0, columns - value.shape[1])))


def body(
    hidden, lengths, pre_gain, w_zx, w_bc, w_dt, conv_x, conv_bc, head_params,
    norm_gain, w_out, cotangent,
):
    seqs, cores, parts = (lax.axis_size(a) for a in ("seq", "tensor", "dp"))
    place, core = lax.axis_index("seq"), lax.axis_index("tensor")
    piece, width = hidden.shape[1], hidden.shape[2]
    tokens, share = piece * seqs, piece // cores
    depth = w_zx.shape[1]
    inner = w_zx.shape[3] // seqs
    heads = w_dt.shape[2] // seqs
    pair_cols = w_bc.shape[2]
    bc_at = 2 * inner
    step_at = bc_at + -(-pair_cols // LANES) * LANES
    slab_cols = step_at + LANES
    sizes = (tokens, inner, heads, step_at)
    live = (jnp.arange(tokens, dtype=jnp.int32) < lengths[0]).astype(F32)[:, None]

    slabs, mixes = [], []
    for layer in range(L):
        wide = w_zx[layer].reshape(depth, 2, seqs, inner).transpose(2, 0, 1, 3)
        wide = wide.reshape(seqs, depth, 2 * inner)
        pair_part = jnp.broadcast_to(w_bc[layer][None], (seqs, depth, pair_cols))
        pair_part = jnp.pad(pair_part, ((0, 0), (0, 0), (0, step_at - bc_at - pair_cols)))
        step_part = w_dt[layer].reshape(depth, seqs, heads).transpose(1, 0, 2)
        step_part = jnp.pad(step_part, ((0, 0), (0, 0), (0, LANES - heads)))
        slab = exchange_axis(jnp.concatenate([wide, pair_part, step_part], axis=2), "seq")
        slabs.append(gather_axis(slab, "dp").reshape(width, slab_cols))
        mix = exchange_axis(w_out[layer].reshape(seqs, inner, depth), "seq")
        mix = gather_axis(mix, "dp").reshape(parts * seqs, inner, depth)
        mixes.append(mix.transpose(1, 0, 2).reshape(inner, width))

    def own_rows(value):
        return lax.dynamic_slice_in_dim(value[0], core * share, share, 0)

    residual = own_rows(hidden).astype(F32)
    upstream_low = own_rows(cotangent)
    upstream = upstream_low.astype(F32)
    upstream_full = gather_rows(upstream_low)

    def tensor_columns(value):
        parts_of = gather_axis(value, "tensor")
        return jnp.moveaxis(parts_of, 0, 1).reshape(value.shape[0], -1)

    kept = []
    for layer in range(L):
        conv = pad_to(
            lax.dynamic_slice_in_dim(conv_x[layer], place * inner, inner, 1), 8, inner
        )
        head_rows = pad_to(
            lax.dynamic_slice_in_dim(head_params[layer], place * heads, heads, 1), 8, LANES
        )
        gain = lax.dynamic_slice_in_dim(norm_gain[layer], place * inner, inner, 0)[None]
        entry = residual
        normed = gather_rows(prenorm(residual, pre_gain[layer]).astype(BF16))
        proj = jnp.dot(normed, slabs[layer], preferred_element_type=F32)
        pair_raw = (proj[:, bc_at : bc_at + pair_cols] * live).astype(BF16)
        padded_pair = jnp.pad(pair_raw.astype(F32), ((K - 1, 0), (0, 0)))
        pairs = tensor_columns(conv_silu(padded_pair, conv_bc[layer]).astype(BF16))
        outputs, mixed, inputs, states, squares = run_forward(
            sizes, lengths, proj, pairs, conv, head_rows, gain
        )
        squares = sum_axis(sum_axis(squares, "tensor"), "seq").reshape(tokens)
        scale = lax.rsqrt(squares / DI + EPSILON)
        own_scale = lax.dynamic_slice_in_dim(scale, (place * cores + core) * share, share, 0)
        branch = scatter_rows(jnp.dot(mixed, mixes[layer], preferred_element_type=F32))
        branch = branch * own_scale[:, None]
        residual = residual + branch
        kept.append(
            (entry, branch, normed, proj, padded_pair, pairs, outputs, inputs, states, scale,
             own_scale, conv, head_rows, gain)
        )
    result_low = residual.astype(BF16)

    shared, owned, pair_convs = [None] * L, [None] * L, [None] * L
    slab_grads, mix_grads = [None] * L, [None] * L
    for layer in reversed(range(L)):
        (entry, branch, normed, proj, padded_pair, pairs, outputs, inputs, states, scale,
         own_scale, conv, head_rows, gain) = kept[layer]
        along = jnp.sum(upstream_low.astype(F32) * branch, axis=-1) / own_scale
        along = gather_rows(along)
        mixgrad = lax.dot_general(
            upstream_full, mixes[layer], (NT, ((), ())), preferred_element_type=F32
        )
        scale_wide = jnp.broadcast_to(scale[:, None], (tokens, LANES))
        coef_wide = jnp.broadcast_to((scale**3 * along / DI)[:, None], (tokens, LANES))
        mixed_in, slab, bc, conv_grad, head_grad, small = run_backward(
            sizes, lengths, proj, pairs, conv, head_rows, gain, inputs, outputs, states,
            mixgrad, scale_wide, coef_wide,
        )
        mix_grad = lax.dot_general(
            mixed_in, upstream_full, (TN, ((), ())), preferred_element_type=F32
        )
        bc = jnp.moveaxis(bc.reshape(tokens, cores, pair_cols), 1, 0)
        bc = sum_axis(scatter_axis(bc, "tensor", F32), "seq", BF16)
        unused, pull_pair = jax.vjp(conv_silu, padded_pair, conv_bc[layer])
        d_padded, d_conv_bc = pull_pair(bc)
        d_pair = (d_padded[K - 1 :] * live).astype(BF16)
        slab = lax.dynamic_update_slice_in_dim(
            slab, pad_to(d_pair / seqs, tokens, step_at - bc_at), bc_at, 1
        )
        partial = lax.dot_general(
            slab, slabs[layer], (NT, ((), ())), preferred_element_type=F32
        )
        own = scatter_rows(partial)
        slab_grad = lax.dot_general(normed, slab, (TN, ((), ())), preferred_element_type=F32)
        slab_grad = scatter_axis(slab_grad.reshape(parts, seqs, depth, slab_cols), "dp")
        slab_grads[layer] = exchange_axis(slab_grad.astype(BF16), "seq").astype(F32)
        mix_grad = mix_grad.reshape(inner, parts, seqs, depth).transpose(1, 2, 0, 3)
        mix_grad = scatter_axis(mix_grad, "dp")
        mix_grads[layer] = exchange_axis(mix_grad.astype(BF16), "seq").astype(F32)
        unused, pull_norm = jax.vjp(prenorm, entry, pre_gain[layer])
        d_entry, d_pre = pull_norm(own)
        upstream = upstream + d_entry
        upstream_low = upstream.astype(BF16)
        if layer > 0:
            upstream_full = gather_rows(upstream_low)
        skip = small[1].reshape(heads, P_SIZE).sum(-1)
        shared[layer] = d_pre
        pair_convs[layer] = d_conv_bc
        owned[layer] = jnp.concatenate(
            [conv_grad[: K + 1].reshape(-1), small[0], head_grad[:2, :heads].reshape(-1), skip]
        )

    result = jnp.swapaxes(gather_axis(result_low, "tensor"), 0, 0).reshape(piece, width)
    d_hidden = gather_axis(upstream, "tensor").reshape(piece, width)
    d_pre = jnp.stack(shared)
    for axis in ("dp", "seq", "tensor"):
        d_pre = sum_axis(d_pre, axis)
    small_sums = sum_axis(jnp.stack(owned), "dp")
    small_all = jnp.moveaxis(gather_axis(small_sums, "seq"), 0, 1)
    pair_sums = sum_axis(jnp.stack(pair_convs), "dp")

    def columns(first, count, each):
        part = small_all[:, :, first : first + count * each].reshape(L, seqs, count, each)
        return part.transpose(0, 2, 1, 3).reshape(L, count, seqs * each)

    edge = (K + 1) * inner
    slab_all = jnp.stack(slab_grads)
    d_zx = slab_all[..., :bc_at].reshape(L, seqs, depth, 2, inner).transpose(0, 2, 3, 1, 4)
    d_bc = slab_all[..., bc_at : bc_at + pair_cols].sum(1)
    d_dt = slab_all[..., step_at : step_at + heads].transpose(0, 2, 1, 3)
    return (
        result[None],
        d_hidden[None],
        d_pre,
        d_zx.reshape(L, depth, 2, seqs * inner),
        d_bc,
        d_dt.reshape(L, depth, seqs * heads),
        columns(0, K + 1, inner),
        pair_sums,
        columns(edge + inner, 3, heads),
        columns(edge, 1, inner)[:, 0],
        jnp.stack(mix_grads).reshape(L, seqs * inner, depth),
    )


def solution(mesh):
    wide = P(None, ("dp", "seq"), None, "tensor")
    thin = P(None, ("dp", "seq"), "tensor")
    rows = P("dp", "seq", None)
    flat = P(None, None, "tensor")
    gain = P(None, "tensor")
    mix = P(None, "tensor", ("dp", "seq"))
    return jax.shard_map(
        body,
        mesh=mesh,
        in_specs=(rows, P("dp"), P(), wide, thin, thin, flat, flat, flat, gain, mix, rows),
        out_specs=(rows, rows, P(), wide, thin, thin, flat, flat, flat, gain, mix),
        check_vma=False,
    )
```

```python
import functools

import jax
import jax.numpy as jnp
from jax import lax
from jax.experimental import pallas as pl
from jax.experimental.pallas import tpu as pltpu
from jax.sharding import PartitionSpec as P

DI = 4096
P_SIZE = 64
N = 128
K = 4
Q = 256
L = 2
LANES = 128
EPSILON = 1e-05
CHUNK = 32
LAG = 2
F32 = jnp.float32
BF16 = jnp.bfloat16
PRECISE = lax.Precision.HIGHEST


def swap(value, axis, distance):
    size = lax.axis_size(axis)
    return lax.ppermute(value, axis, [(i, i ^ distance) for i in range(size)])


def pick(value, index):
    return lax.dynamic_index_in_dim(value, index, 0, False)


def put(buffer, value, index):
    return lax.dynamic_update_index_in_dim(buffer, value, index, 0)


def gather_axis(value, axis):
    size, place = lax.axis_size(axis), lax.axis_index(axis)
    out = put(jnp.zeros((size,) + value.shape, value.dtype), value, place)
    for distance in range(1, size):
        out = put(out, swap(value, axis, distance), place ^ distance)
    return out


def exchange_axis(values, axis):
    size, place = lax.axis_size(axis), lax.axis_index(axis)
    out = put(jnp.zeros_like(values), pick(values, place), place)
    for distance in range(1, size):
        out = put(out, swap(pick(values, place ^ distance), axis, distance), place ^ distance)
    return out


def scatter_axis(values, axis, kind=BF16):
    size, place = lax.axis_size(axis), lax.axis_index(axis)
    total = pick(values, place).astype(F32)
    for distance in range(1, size):
        sent = pick(values, place ^ distance).astype(kind)
        total = total + swap(sent, axis, distance).astype(F32)
    return total


def sum_axis(value, axis, kind=F32):
    size = lax.axis_size(axis)
    distance = 1
    while distance < size:
        value = value + swap(value.astype(kind), axis, distance).astype(value.dtype)
        distance *= 2
    return value


def gather_rows(own):
    along = gather_axis(own, "seq")
    both = jnp.swapaxes(gather_axis(along, "tensor"), 0, 1)
    return both.reshape((-1,) + own.shape[1:])


def scatter_rows(partial):
    seqs, cores = lax.axis_size("seq"), lax.axis_size("tensor")
    parts = partial.reshape((seqs, cores, -1) + partial.shape[1:])
    halves = scatter_axis(jnp.swapaxes(parts, 0, 1), "tensor")
    return scatter_axis(halves, "seq")


def lane_iota(shape):
    return lax.broadcasted_iota(jnp.int32, shape, len(shape) - 1)


def row_iota(shape):
    return lax.broadcasted_iota(jnp.int32, shape, len(shape) - 2)


def dot(a, b, dims, precision=None):
    return lax.dot_general(
        a, b, (dims, ((), ())), preferred_element_type=F32, precision=precision
    )


NN = ((1,), (0,))
NT = ((1,), (1,))
TN = ((0,), (0,))


def pair_of(columns, j):
    rows = columns.shape[0]
    first = lane_iota((rows, LANES)) < P_SIZE
    return jnp.where(first, columns[:, 2 * j : 2 * j + 1], columns[:, 2 * j + 1 : 2 * j + 2])


def spread(columns, heads):
    return jnp.concatenate([pair_of(columns, j) for j in range(heads // 2)], axis=1)


def split_pair(pair):
    first = lane_iota(pair.shape) < P_SIZE
    zero = jnp.zeros_like(pair)
    return jnp.where(first, pair, zero), jnp.where(first, zero, pair)


def block_steps(raw, head_rows, live):
    steps = jax.nn.softplus(raw + head_rows[1:2]) * live
    rate = -jnp.exp(head_rows[0:1])
    return steps, rate


def sigmoid(v):
    return 1.0 / (1.0 + jnp.exp(-v))


def forward_kernel(
    sizes, length_ref, proj_ref, pairs_ref, conv_ref, head_ref, gain_ref,
    outputs_ref, mixed_ref, inputs_ref, states_ref, square_ref, state, halo,
):
    tokens, inner, heads, step_at = sizes
    head_rows = head_ref[...]
    head_lane = lane_iota((1, LANES)) < heads
    causal = row_iota((Q, Q)) >= lane_iota((Q, Q))
    below = causal.astype(F32)
    state[...] = jnp.zeros_like(state)
    halo[...] = jnp.zeros_like(halo)
    length = length_ref[0]

    def block(k, carry):
        start = pl.multiple_of(k * Q, Q)
        rows = pl.ds(start, Q)
        live = (row_iota((Q, 1)) + start < length).astype(F32)
        raw = (proj_ref[rows, inner : 2 * inner].astype(F32) * live).astype(BF16).astype(F32)
        padded = jnp.concatenate([halo[...], raw], axis=0)
        halo[...] = raw[Q - 8 :]
        pre = conv_ref[K : K + 1, :]
        for tap in range(K):
            pre = pre + conv_ref[tap : tap + 1, :] * padded[5 + tap : 5 + tap + Q]
        inputs = (pre * sigmoid(pre)).astype(BF16)
        inputs_ref[rows, :] = inputs
        steps, rate = block_steps(proj_ref[rows, step_at : step_at + LANES], head_rows, live)
        decay = jnp.where(head_lane, steps * rate, 0.0)
        cum = dot(below, decay, NN, PRECISE)
        cum_t = cum.T
        b_rows = pairs_ref[rows, :N]
        c_rows = pairs_ref[rows, N:]
        scores = jnp.where(causal, dot(c_rows, b_rows, NT), 0.0)
        before = state[...]
        states_ref[k] = before
        inputs_f = inputs.astype(F32)
        scaled = inputs_f * spread(steps, heads)
        scaled_low = scaled.astype(BF16)
        across = dot(c_rows, before.astype(BF16), NT) * spread(jnp.exp(cum), heads)
        last = cum[Q - 1 : Q]
        tail = jnp.exp(last - cum)
        square = jnp.zeros((Q, 1), F32)
        for j in range(heads // 2):
            cols = slice(j * LANES, (j + 1) * LANES)
            mixing = []
            for h in (2 * j, 2 * j + 1):
                gap = jnp.minimum(cum[:, h : h + 1] - cum_t[h : h + 1, :], 0.0)
                mixing.append((jnp.exp(gap) * scores).astype(BF16))
            both = jnp.concatenate(mixing, axis=1)
            stacked = jnp.concatenate(split_pair(scaled_low[:, cols]), axis=0)
            out = dot(both, stacked, NN) + across[:, cols]
            out = out + pair_of(head_rows[2:3], j) * inputs_f[:, cols]
            outputs_ref[rows, cols] = out
            gate = proj_ref[rows, cols]
            gated = out * gate * sigmoid(gate)
            mixed_ref[rows, cols] = (gated * gain_ref[:, cols]).astype(BF16)
            square = square + jnp.sum(gated * gated, axis=1, keepdims=True)
        square_ref[rows, :] = jnp.broadcast_to(square, (Q, LANES))
        fresh = dot((scaled * spread(tail, heads)).astype(BF16), b_rows, TN)
        for h in range(heads):
            own = slice(h * P_SIZE, (h + 1) * P_SIZE)
            state[own, :] = jnp.exp(last[:, h : h + 1]) * before[own] + fresh[own]
        return carry

    lax.fori_loop(0, tokens // Q, block, 0)


def backward_kernel(
    sizes, length_ref, proj_ref, pairs_ref, conv_ref, head_ref, gain_ref, inputs_ref,
    outputs_ref, states_ref, up_ref, mix_ref, extra_ref, up_extra_ref,
    mixed_ref, slab_ref, bc_ref, conv_grad_ref, head_grad_ref, small_ref, state, halo,
    scratch_a, scratch_b, scratch_c, mixgrad_ref,
):
    tokens, inner, heads, step_at = sizes
    head_rows = head_ref[...]
    head_lane = lane_iota((1, LANES)) < heads
    causal = row_iota((Q, Q)) >= lane_iota((Q, Q))
    below = causal.astype(F32)
    onehot = (row_iota((inner, LANES)) // P_SIZE == lane_iota((inner, LANES))).astype(F32)
    state[...] = jnp.zeros_like(state)
    halo[...] = jnp.zeros_like(halo)
    conv_grad_ref[...] = jnp.zeros_like(conv_grad_ref)
    head_grad_ref[...] = jnp.zeros_like(head_grad_ref)
    small_ref[...] = jnp.zeros_like(small_ref)
    length = length_ref[0]
    blocks = tokens // Q

    def block(turn, carry):
        k = blocks - 1 - turn
        start = pl.multiple_of(k * Q, Q)
        rows = pl.ds(start, Q)
        live = (row_iota((Q, 1)) + start < length).astype(F32)
        steps, rate = block_steps(proj_ref[rows, step_at : step_at + LANES], head_rows, live)
        decay = jnp.where(head_lane, steps * rate, 0.0)
        cum = dot(below, decay, NN, PRECISE)
        cum_t = cum.T
        last = cum[Q - 1 : Q]
        grow = jnp.exp(cum)
        tail = jnp.exp(last - cum)
        b_rows = pairs_ref[rows, :N]
        c_rows = pairs_ref[rows, N:]
        scores = jnp.where(causal, dot(c_rows, b_rows, NT), 0.0)
        before = states_ref[k]
        before_low = before.astype(BF16)
        after = state[...]
        after_low = after.astype(BF16)
        scale = joined(extra_ref[rows, :], 0, 3)
        coef = scale * scale * scale * joined(up_extra_ref[rows, :], 3, 2) / DI
        mixgrad = jnp.zeros((Q, inner), F32)
        for n in range(mix_ref.shape[0] // 2):
            wide = jnp.concatenate([mix_ref[2 * n], mix_ref[2 * n + 1]], axis=1)
            step = wide.shape[1]
            mixgrad = mixgrad + dot(up_ref[rows, n * step : (n + 1) * step], wide, NT)
        mixgrad_ref[...] = mixgrad
        spread_b = dot(b_rows, after_low, NT)
        pair_sum = jnp.zeros((Q, Q), F32)
        for j in range(heads // 2):
            cols = slice(j * LANES, (j + 1) * LANES)
            steps_j, grow_j, tail_j = pair_of(steps, j), pair_of(grow, j), pair_of(tail, j)
            skip_j = pair_of(head_rows[2:3], j)
            gate = proj_ref[rows, cols]
            sig = sigmoid(gate)
            silu = gate * sig
            out = outputs_ref[rows, cols]
            gated = out * silu
            mixgrad = mixgrad_ref[:, cols]
            gain = gain_ref[:, cols]
            normal = gated * scale
            small_ref[0:1, cols] += jnp.sum(mixgrad * normal, axis=0, keepdims=True)
            mixed_ref[rows, cols] = (normal * gain).astype(BF16)
            d_gated = scale * (mixgrad * gain) - gated * coef
            d_out = d_gated * silu
            slab_ref[rows, cols] = (
                d_gated * out * sig * (1.0 + gate * (1.0 - sig))
            ).astype(BF16)
            d_low = d_out.astype(BF16)
            inputs = inputs_ref[rows, cols].astype(F32)
            small_ref[1:2, cols] += jnp.sum(d_out * inputs, axis=0, keepdims=True)
            scaled = inputs * steps_j
            scaled_low = scaled.astype(BF16)
            d_halves = split_pair(d_low)
            mixing = []
            for at, h in enumerate((2 * j, 2 * j + 1)):
                gap = jnp.minimum(cum[:, h : h + 1] - cum_t[h : h + 1, :], 0.0)
                fade = jnp.exp(gap)
                mixing.append((fade * scores).astype(BF16))
                pair_sum = pair_sum + fade * dot(d_halves[at], scaled_low, NT)
            y_tail = spread_b[:, cols] * tail_j
            y = dot(jnp.concatenate(mixing, axis=0), jnp.concatenate(d_halves, axis=0), TN)
            y = y + y_tail
            scaled_f = scaled_low.astype(F32)
            scratch_a[:, cols] = inputs * y
            scratch_b[:, cols] = d_low.astype(F32) * (out - skip_j * inputs) - scaled_f * y
            small_ref[2:3, cols] = jnp.sum(scaled_f * y_tail, axis=0, keepdims=True)
            scratch_c[:, cols] = steps_j * y + skip_j * d_out
            mixed_low = (d_out * grow_j).astype(BF16)
            slab_ref[rows, inner + j * LANES : inner + (j + 1) * LANES] = mixed_low
        grown = slab_ref[rows, inner : 2 * inner]
        pair_low = jnp.where(causal, pair_sum, 0.0).astype(BF16)
        tailed = (inputs_ref[rows, :].astype(F32) * spread(steps * tail, heads)).astype(BF16)
        bc_ref[rows, :N] = dot(pair_low, c_rows, TN) + dot(tailed, after_low, NN)
        bc_ref[rows, N:] = dot(pair_low, b_rows, NN) + dot(grown, before_low, NN)
        kept = dot(jnp.ones((8, N), F32), after_low.astype(F32) * before, NT, PRECISE)
        ends = dot(kept, onehot, NN, PRECISE)[0:1] * jnp.exp(last)
        ends = ends + dot(
            jnp.broadcast_to(small_ref[2:3, :], (8, inner)), onehot, NN, PRECISE
        )[0:1]
        d_decay = dot(below, dot(scratch_b[...], onehot, NN, PRECISE), TN, PRECISE) + ends
        d_steps = dot(scratch_a[...], onehot, NN, PRECISE) + rate * d_decay
        d_soft = d_steps * live * sigmoid(
            proj_ref[rows, step_at : step_at + LANES] + head_rows[1:2]
        )
        d_soft = jnp.where(head_lane, d_soft, 0.0)
        slab_ref[rows, step_at : step_at + LANES] = d_soft.astype(BF16)
        head_grad_ref[0:1, :] += rate * jnp.sum(
            jnp.where(head_lane, steps * d_decay, 0.0), axis=0, keepdims=True
        )
        head_grad_ref[1:2, :] += jnp.sum(d_soft, axis=0, keepdims=True)
        gathered = dot(grown, c_rows, TN)
        for h in range(heads):
            own = slice(h * P_SIZE, (h + 1) * P_SIZE)
            state[own, :] = jnp.exp(last[:, h : h + 1]) * after[own] + gathered[own]
        raw = (proj_ref[rows, inner : 2 * inner] * live).astype(BF16).astype(F32)
        ahead = pl.ds(pl.multiple_of(jnp.maximum(start - 8, 0), 8), 8)
        earlier = row_iota((8, 1)) + start - 8
        ahead_live = jnp.logical_and(earlier >= 0, earlier < length).astype(F32)
        first = (proj_ref[ahead, inner : 2 * inner] * ahead_live).astype(BF16).astype(F32)
        padded = jnp.concatenate([first, raw], axis=0)
        pre = conv_ref[K : K + 1, :]
        for tap in range(K):
            pre = pre + conv_ref[tap : tap + 1, :] * padded[5 + tap : 5 + tap + Q]
        sig = sigmoid(pre)
        d_pre = scratch_c[...] * sig * (1.0 + pre * (1.0 - sig))
        after_pre = jnp.concatenate([d_pre, halo[...]], axis=0)
        halo[...] = d_pre[0:8]
        d_raw = jnp.zeros((Q, inner), F32)
        for tap in range(K):
            conv_grad_ref[tap : tap + 1, :] += jnp.sum(
                d_pre * padded[5 + tap : 5 + tap + Q], axis=0, keepdims=True
            )
            d_raw = d_raw + conv_ref[tap : tap + 1, :] * after_pre[3 - tap : 3 - tap + Q]
        conv_grad_ref[K : K + 1, :] += jnp.sum(d_pre, axis=0, keepdims=True)
        slab_ref[rows, inner : 2 * inner] = (d_raw * live).astype(BF16)
        return carry

    lax.fori_loop(0, blocks, block, 0)


VMEM_SPEC = pl.BlockSpec(memory_space=pltpu.VMEM)
SMEM_SPEC = pl.BlockSpec(memory_space=pltpu.SMEM)
PARAMS = pltpu.CompilerParams(vmem_limit_bytes=56 * 1024 * 1024)


def run_forward(sizes, lengths, proj, pairs, conv, heads_in, gain):
    tokens, inner, heads, step_at = sizes
    shapes = (
        jax.ShapeDtypeStruct((tokens, inner), F32),
        jax.ShapeDtypeStruct((tokens, inner), BF16),
        jax.ShapeDtypeStruct((tokens, inner), BF16),
        jax.ShapeDtypeStruct((tokens // Q, inner, N), F32),
        jax.ShapeDtypeStruct((tokens, LANES), F32),
    )
    return pl.pallas_call(
        functools.partial(forward_kernel, sizes),
        out_shape=shapes,
        in_specs=[SMEM_SPEC] + [VMEM_SPEC] * 5,
        out_specs=[VMEM_SPEC] * 5,
        scratch_shapes=[pltpu.VMEM((inner, N), F32), pltpu.VMEM((8, inner), F32)],
        compiler_params=PARAMS,
        cost_estimate=pl.CostEstimate(flops=8 * 10**9, bytes_accessed=16 * 10**6, transcendentals=4 * 10**6),
        name="scan_forward",
    )(lengths, proj, pairs, conv, heads_in, gain)


def run_backward(sizes, lengths, proj, pairs, conv, heads_in, gain, inputs, outputs, states, up, mix, extra, up_extra):
    tokens, inner, heads, step_at = sizes
    width = proj.shape[1]
    shapes = (
        jax.ShapeDtypeStruct((tokens, inner), BF16),
        jax.ShapeDtypeStruct((tokens, width), BF16),
        jax.ShapeDtypeStruct((tokens, 2 * N), F32),
        jax.ShapeDtypeStruct((8, inner), F32),
        jax.ShapeDtypeStruct((8, LANES), F32),
        jax.ShapeDtypeStruct((8, inner), F32),
    )
    return pl.pallas_call(
        functools.partial(backward_kernel, sizes),
        out_shape=shapes,
        in_specs=[SMEM_SPEC] + [VMEM_SPEC] * 12,
        out_specs=[VMEM_SPEC] * 6,
        scratch_shapes=[
            pltpu.VMEM((inner, N), F32),
            pltpu.VMEM((8, inner), F32),
        ]
        + [pltpu.VMEM((Q, inner), F32)] * 4,
        compiler_params=PARAMS,
        cost_estimate=pl.CostEstimate(flops=20 * 10**9, bytes_accessed=24 * 10**6, transcendentals=6 * 10**6),
        name="scan_backward",
    )(lengths, proj, pairs, conv, heads_in, gain, inputs, outputs, states, up, mix, extra, up_extra)


def joined(extra, first, count):
    total = extra[:, first : first + 1].astype(F32)
    for lane in range(first + 1, first + count):
        total = total + extra[:, lane : lane + 1].astype(F32)
    return total


def parted(columns):
    rows = columns[0][0].shape[0]
    lane = lane_iota((rows, LANES))
    out = jnp.zeros((rows, LANES), F32)
    for value, first, count in columns:
        rest = value
        for at in range(count):
            part = rest.astype(BF16).astype(F32)
            out = jnp.where(lane == first + at, part, out)
            rest = rest - part
    return out.astype(BF16)


def reduce_kernel(mode, dims, *refs):
    seqs, cores, tokens, width, share, chunk = dims
    forward, last = mode.startswith("forward"), mode.endswith("last")
    refs = list(refs)
    take = lambda count: [refs.pop(0) for _ in range(count)]
    lhs_ref, rhs_ref, gain_ref = take(3)
    if forward:
        square_ref, res_ref = take(2)
        up_ref = take(1)[0] if last else None
    else:
        res_ref, up_ref = take(2)
        raw_ref = None if last else take(1)[0]
    full_ref = None if mode == "backward_last" else take(1)[0]
    if last:
        own_ref = take(1)[0]
    if forward:
        if not last:
            new_ref, raw_out = take(2)
    else:
        gain_out = take(1)[0]
        if not last:
            new_ref = take(1)[0]
    stage, core_recv, send, recv = take(4)
    if last:
        hold = take(1)[0]
    core_ss, core_rs, ss, rs, ag_ss, ag_rs, sib_ss, sib_rs, own_ss, own_rs = take(10)

    place, core = lax.axis_index("seq"), lax.axis_index("tensor")
    half, piece, pieces = tokens // 2, share * cores, seqs // 2
    rows_own = share * pieces
    per_piece = share // chunk
    chunks = rows_own // chunk
    pos = {1: place, 0: seqs - 1 - place}
    step = {1: 1, 0: -1}
    mesh_id = pl.DeviceIdType.MESH

    barrier = pltpu.get_barrier_semaphore()
    for a in range(seqs):
        for b in range(cores):
            if a or b:
                peer = {"seq": lax.rem(place + a, seqs), "tensor": lax.rem(core + b, cores)}
                pl.semaphore_signal(barrier, inc=1, device_id=peer, device_id_type=mesh_id)
    pl.semaphore_wait(barrier, seqs * cores - 1)

    def piece_at(direction, p):
        return p if direction else pieces - 1 - p

    def start_of(direction, at_core, j):
        p, inside = j // per_piece, lax.rem(j, per_piece)
        base = direction * half + piece_at(direction, p) * piece
        return pl.multiple_of(base + at_core * share + inside * chunk, chunk)

    tile = 256
    for direction in (1, 0):
        lhs_rows = slice(direction * half, (direction + 1) * half)

        def columns(n, carry):
            at = pl.ds(pl.multiple_of(n * tile, tile), tile)
            lhs = lhs_ref[lhs_rows, :]
            if forward:
                wide = jnp.concatenate([rhs_ref[2 * n], rhs_ref[2 * n + 1]], axis=1)
                value = dot(lhs, wide, NN)
            else:
                value = dot(lhs, rhs_ref[at, :], NT)
            value = value.astype(BF16)
            for p in range(pieces):
                for b in range(cores):
                    first = piece_at(direction, p) * piece + b * share
                    stage[b, direction, p * share : (p + 1) * share, at] = value[
                        first : first + share
                    ]
            return carry

        lax.fori_loop(0, width // tile, columns, 0)
        if forward:
            for p in range(pieces):
                for b in range(cores):
                    first = direction * half + piece_at(direction, p) * piece + b * share
                    stage[b, direction, p * share : (p + 1) * share, width:] = parted(
                        [(square_ref[first : first + share, 0:1], 0, 2)]
                    )
        for o in range(1, cores):
            core_copy(stage, core_recv, core_ss, core_rs, core, cores, o, direction).start()

    def chain_copy(direction, j):
        rows = pl.ds(pl.multiple_of(j * chunk, chunk), chunk)
        return pltpu.make_async_remote_copy(
            src_ref=send.at[direction, rows], dst_ref=recv.at[direction, rows],
            send_sem=ss.at[direction, j], recv_sem=rs.at[direction, j],
            device_id={"seq": place + step[direction]}, device_id_type=mesh_id,
        )

    def back_copy(direction, j):
        rows = pl.ds(start_of(direction, core, j), chunk)
        return pltpu.make_async_remote_copy(
            src_ref=full_ref.at[rows], dst_ref=full_ref.at[rows],
            send_sem=ag_ss.at[direction, j], recv_sem=ag_rs.at[direction, j],
            device_id={"seq": place - step[direction]}, device_id_type=mesh_id,
        )

    def side_copy(direction, j, o, at_core):
        rows = pl.ds(start_of(direction, at_core, j), chunk)
        return pltpu.make_async_remote_copy(
            src_ref=full_ref.at[rows], dst_ref=full_ref.at[rows],
            send_sem=sib_ss.at[o - 1, direction, j], recv_sem=sib_rs.at[o - 1, direction, j],
            device_id={"tensor": lax.rem(core + o, cores)}, device_id_type=mesh_id,
        )

    def own_copy(direction, j):
        inside = lax.rem(j, per_piece)
        rows = pl.ds(pl.multiple_of(j * chunk, chunk), chunk)
        to = direction * pieces + piece_at(direction, j // per_piece)
        return pltpu.make_async_remote_copy(
            src_ref=hold.at[rows],
            dst_ref=own_ref.at[pl.ds(pl.multiple_of(inside * chunk, chunk), chunk)],
            send_sem=own_ss.at[j], recv_sem=own_rs.at[inside],
            device_id={"seq": to}, device_id_type=mesh_id,
        )

    def spread_out(direction, j):
        back_copy(direction, j).start()
        for o in range(1, cores):
            side_copy(direction, j, o, core).start()

    if not forward:
        gain_out[...] = jnp.zeros_like(gain_out)

    def finish(direction, j, total):
        rows = pl.ds(pl.multiple_of(j * chunk, chunk), chunk)
        out_rows = pl.ds(start_of(direction, core, j), chunk)
        gain = gain_ref[...]
        residual = res_ref[rows, :]
        if forward:
            square = total[:, width : width + 1] + total[:, width + 1 : width + 2]
            scale = lax.rsqrt(square / DI + EPSILON)
            raw = total[:, :width]
            value = residual + raw * scale
            if last:
                along = jnp.sum(up_ref[rows, :].astype(F32) * raw, axis=1, keepdims=True)
                full_ref[out_rows, :] = parted([(scale, 0, 3), (along, 3, 2)])
                result = value.astype(BF16)
            else:
                new_ref[rows, :] = value
                raw_out[rows, :] = raw
                mean = jnp.sum(value * value, axis=1, keepdims=True) / width
                full_ref[out_rows, :width] = (value * lax.rsqrt(mean + EPSILON) * gain).astype(BF16)
                full_ref[out_rows, width:] = parted([(scale, 0, 3)])
        else:
            mean = jnp.sum(residual * residual, axis=1, keepdims=True) / width
            q = lax.rsqrt(mean + EPSILON)
            scaled = total * gain
            gain_out[0:1, :] += jnp.sum(total * residual * q, axis=0, keepdims=True)
            along = jnp.sum(scaled * residual, axis=1, keepdims=True) / width
            value = up_ref[rows, :].astype(F32) + q * scaled - residual * (q * q * q * along)
            if last:
                result = value
            else:
                new_ref[rows, :] = value
                low = value.astype(BF16)
                full_ref[out_rows, :width] = low
                along = jnp.sum(low.astype(F32) * raw_ref[rows, :], axis=1, keepdims=True)
                full_ref[out_rows, width:] = parted([(along, 3, 2)])
        if full_ref is not None:
            spread_out(direction, j)
        if last:
            to = direction * pieces + piece_at(direction, j // per_piece)
            inside = pl.ds(pl.multiple_of(lax.rem(j, per_piece) * chunk, chunk), chunk)

            @pl.when(to == place)
            def _():
                own_ref[inside, :] = result

            @pl.when(to != place)
            def _():
                hold[rows, :] = result
                own_copy(direction, j).start()

    for o in range(1, cores):
        for direction in (1, 0):
            core_copy(stage, core_recv, core_ss, core_rs, core, cores, o, direction).wait()

    def chain(turn, carry):
        for direction in (1, 0):
            j = turn - LAG * pos[direction]
            rows = pl.ds(pl.multiple_of(j * chunk, chunk), chunk)
            due = jnp.logical_and(j >= 0, j < chunks)

            def local():
                value = stage[core, direction, rows, :].astype(F32)
                for o in range(1, cores):
                    value = value + core_recv[o - 1, direction, rows, :].astype(F32)
                return value

            def joint():
                chain_copy(direction, j).wait_recv()
                return local() + recv[direction, rows, :].astype(F32)

            def pass_on(value):
                if forward:
                    square = value[:, width : width + 1] + value[:, width + 1 : width + 2]
                    send[direction, rows, :width] = value[:, :width].astype(BF16)
                    send[direction, rows, width:] = parted([(square, 0, 2)])
                else:
                    send[direction, rows, :] = value.astype(BF16)
                chain_copy(direction, j).start()

            @pl.when(jnp.logical_and(due, pos[direction] == 0))
            def _():
                pass_on(local())

            inside = jnp.logical_and(pos[direction] > 0, pos[direction] < seqs - 1)

            @pl.when(jnp.logical_and(due, inside))
            def _():
                pass_on(joint())

            @pl.when(jnp.logical_and(due, pos[direction] == seqs - 1))
            def _():
                finish(direction, j, joint())

        return carry

    lax.fori_loop(0, chunks + LAG * (seqs - 1), chain, 0)

    if full_ref is not None:

        def back(turn, carry):
            for direction in (1, 0):
                away = seqs - 1 - pos[direction]
                j = turn - LAG * (away - 1)
                due = jnp.logical_and(j >= 0, j < chunks)

                @pl.when(jnp.logical_and(due, away > 0))
                def _():
                    back_copy(direction, j).wait_recv()

                    @pl.when(pos[direction] > 0)
                    def _():
                        back_copy(direction, j).start()

                    for o in range(1, cores):
                        side_copy(direction, j, o, core).start()

            return carry

        lax.fori_loop(0, chunks + LAG * (seqs - 2), back, 0)

    def drain(j, carry):
        for direction in (1, 0):

            @pl.when(pos[direction] < seqs - 1)
            def _():
                chain_copy(direction, j).wait_send()

            if full_ref is not None:

                @pl.when(pos[direction] > 0)
                def _():
                    back_copy(direction, j).wait_send()

                for o in range(1, cores):
                    side_copy(direction, j, o, core).wait_send()
                    side_copy(direction, j, o, lax.rem(core - o + cores, cores)).wait_recv()
            if last:
                to = direction * pieces + piece_at(direction, j // per_piece)

                @pl.when(jnp.logical_and(pos[direction] == seqs - 1, to != place))
                def _():
                    own_copy(direction, j).wait_send()

        return carry

    lax.fori_loop(0, chunks, drain, 0)
    if last:

        @pl.when(jnp.logical_and(place > 0, place < seqs - 1))
        def _():
            def arrived(j, carry):
                own_copy(0, j).wait_recv()
                return carry

            lax.fori_loop(0, per_piece, arrived, 0)


def core_copy(stage, core_recv, core_ss, core_rs, core, cores, o, direction):
    to = lax.rem(core + o, cores)
    return pltpu.make_async_remote_copy(
        src_ref=stage.at[to, direction], dst_ref=core_recv.at[o - 1, direction],
        send_sem=core_ss.at[o - 1, direction], recv_sem=core_rs.at[o - 1, direction],
        device_id={"tensor": to}, device_id_type=pl.DeviceIdType.MESH,
    )


def run_reduce(mode, ident, lhs, rhs, gain, more):
    forward, last = mode.startswith("forward"), mode.endswith("last")
    seqs, cores = lax.axis_size("seq"), lax.axis_size("tensor")
    tokens, width = lhs.shape[0], gain.shape[1]
    share = tokens // (seqs * cores)
    chunk = min(CHUNK, share)
    dims = (seqs, cores, tokens, width, share, chunk)
    rows_own = share * seqs // 2
    chunks = rows_own // chunk
    full_width = width + LANES
    shapes = []
    if mode != "backward_last":
        shapes.append(jax.ShapeDtypeStruct((tokens, LANES if last else full_width), BF16))
    if last:
        shapes.append(jax.ShapeDtypeStruct((share, width), BF16 if forward else F32))
    if forward and not last:
        shapes += [jax.ShapeDtypeStruct((rows_own, width), F32)] * 2
    if not forward:
        shapes.append(jax.ShapeDtypeStruct((8, width), F32))
        if not last:
            shapes.append(jax.ShapeDtypeStruct((rows_own, width), F32))
    moved = full_width if forward else width
    siblings = cores - 1
    sem = pltpu.SemaphoreType.DMA
    scratch = [
        pltpu.VMEM((cores, 2, rows_own, moved), BF16),
        pltpu.VMEM((siblings, 2, rows_own, moved), BF16),
        pltpu.VMEM((2, rows_own, moved), BF16),
        pltpu.VMEM((2, rows_own, moved), BF16),
    ]
    if last:
        scratch.append(pltpu.VMEM((rows_own, width), BF16 if forward else F32))
    scratch += [
        sem((siblings, 2)), sem((siblings, 2)), sem((2, chunks)), sem((2, chunks)),
        sem((2, chunks)), sem((2, chunks)), sem((siblings, 2, chunks)), sem((siblings, 2, chunks)),
        sem((chunks,)), sem((max(share // chunk, 1),)),
    ]
    return pl.pallas_call(
        functools.partial(reduce_kernel, mode, dims),
        out_shape=shapes,
        in_specs=[VMEM_SPEC] * (3 + len(more)),
        out_specs=[VMEM_SPEC] * len(shapes),
        scratch_shapes=scratch,
        compiler_params=pltpu.CompilerParams(
            vmem_limit_bytes=56 * 1024 * 1024, collective_id=ident, has_side_effects=True
        ),
        name=mode,
    )(lhs, rhs, gain, *more)


def begin_kernel(dims, slab_ref, mix_ref, rows_ref, slab_out, mix_out, rows_out, *sems):
    seqs, cores, share, chunk = dims
    ex_ss, ex_rs, near_ss, near_rs, far_ss, far_rs, ag_ss, ag_rs, sib_ss, sib_rs, here = sems
    place, core, part = (lax.axis_index(a) for a in ("seq", "tensor", "dp"))
    mesh_id = pl.DeviceIdType.MESH
    near = {1: part + 1 - 2 * lax.rem(part, 2), 2: lax.rem(part + 2, 4)}
    barrier = pltpu.get_barrier_semaphore()
    peers = [{"dp": near[1]}, {"dp": near[2]}]
    for a in range(seqs):
        for b in range(cores):
            if a or b:
                peers.append(
                    {"seq": lax.rem(place + a, seqs), "tensor": lax.rem(core + b, cores)}
                )
    for peer in peers:
        pl.semaphore_signal(barrier, inc=1, device_id=peer, device_id_type=mesh_id)
    pl.semaphore_wait(barrier, len(peers))
    arrays = ((slab_ref, slab_out), (mix_ref, mix_out))

    def remote(source, target, send_sem, recv_sem, device):
        return pltpu.make_async_remote_copy(
            src_ref=source, dst_ref=target, send_sem=send_sem, recv_sem=recv_sem,
            device_id=device, device_id_type=mesh_id,
        )

    def exchange(which, o):
        source, target = arrays[which]
        to = lax.rem(place + o, seqs)
        return remote(
            source.at[to], target.at[part, place], ex_ss.at[which, o - 1], ex_rs.at[which, o - 1],
            {"seq": to},
        )

    def arrive(which, o):
        return lax.rem(place - o + seqs, seqs)

    def to_near(which, o, bit):
        target = arrays[which][1].at[part, arrive(which, o)]
        return remote(
            target, target, near_ss.at[which, o, bit - 1], near_rs.at[which, o, bit - 1],
            {"dp": near[bit]},
        )

    def to_far(which, o):
        bit = 1 + o % 2
        target = arrays[which][1].at[near[bit], arrive(which, o)]
        return remote(
            target, target, far_ss.at[which, o], far_rs.at[which, o], {"dp": near[3 - bit]}
        )

    def block_rows(at_place, at_core, k):
        start = (at_place * cores + at_core) * share + k * chunk
        return pl.ds(pl.multiple_of(start, chunk), chunk)

    def along(direction, d, k):
        target = rows_out.at[block_rows(place - direction * d, core, k)]
        at = (direction + 1) // 2
        return remote(
            target, target, ag_ss.at[at, d, k], ag_rs.at[at, d, k], {"seq": place + direction}
        )

    def beside(direction, d, k, o, at_core):
        target = rows_out.at[block_rows(place - direction * d, at_core, k)]
        at = (direction + 1) // 2
        return remote(
            target, target, sib_ss.at[at, d, k, o - 1], sib_rs.at[at, d, k, o - 1],
            {"tensor": lax.rem(core + o, cores)},
        )

    chunks = share // chunk
    for o in range(1, seqs):
        exchange(0, o).start()
    own = [
        pltpu.make_async_copy(rows_ref, rows_out.at[block_rows_all(place, core, cores, share)], here.at[0])
    ] + [
        pltpu.make_async_copy(
            arrays[which][0].at[place], arrays[which][1].at[part, place], here.at[1 + which]
        )
        for which in (0, 1)
    ]
    for copy in own:
        copy.start()
    for copy in own:
        copy.wait()

    def can(direction):
        return place < seqs - 1 if direction > 0 else place > 0

    def exists(direction, d):
        return place - d >= 0 if direction > 0 else place + d < seqs

    for k in range(chunks):
        for direction in (1, -1):

            @pl.when(can(direction))
            def _():
                along(direction, 0, k).start()

        for o in range(1, cores):
            beside(1, 0, k, o, core).start()
    for o in range(1, seqs):
        exchange(1, o).start()
    for bit in (1, 2):
        to_near(0, 0, bit).start()
    for o in range(1, seqs):
        exchange(0, o).wait_recv()
        for bit in (1, 2):
            to_near(0, o, bit).start()
    def rows_from(d):
        def pass_on(k, carry):
            for direction in (1, -1):

                @pl.when(exists(direction, d))
                def _():
                    along_in(along, direction, d, k)

                    @pl.when(can(direction))
                    def _():
                        along(direction, d, k).start()

                    for o in range(1, cores):
                        beside(direction, d, k, o, core).start()

            return carry

        lax.fori_loop(0, chunks, pass_on, 0)

    def far(which, o):
        for bit in (1, 2):
            from_near(to_near, which, o, bit)
        to_far(which, o).start()

    rows_from(1)
    far(0, 0)
    far(0, 1)
    for bit in (1, 2):
        to_near(1, 0, bit).start()
    for o in range(2, seqs):
        rows_from(o)
        far(0, o)
    for o in range(1, seqs):
        exchange(1, o).wait_recv()
        for bit in (1, 2):
            to_near(1, o, bit).start()
    for o in range(seqs):
        far(1, o)
    for which in (0, 1):
        for o in range(seqs):
            to_far(which, o).wait()
            for bit in (1, 2):
                to_near(which, o, bit).wait_send()
            if o:
                exchange(which, o).wait_send()

    def drain(k, carry):
        for d in range(seqs):
            for direction in (1, -1):

                @pl.when(jnp.logical_and(exists(direction, d), can(direction)))
                def _():
                    along(direction, d, k).wait_send()

                if d > 0 or direction > 0:

                    @pl.when(exists(direction, d))
                    def _():
                        for o in range(1, cores):
                            beside(direction, d, k, o, core).wait_send()
                            beside(direction, d, k, o, lax.rem(core - o + cores, cores)).wait_recv()

        return carry

    lax.fori_loop(0, chunks, drain, 0)


def block_rows_all(place, core, cores, share):
    return pl.ds(pl.multiple_of((place * cores + core) * share, share), share)


def from_near(to_near, which, o, bit):
    to_near(which, o, bit).wait_recv()


def along_in(along, direction, d, k):
    along(direction, d - 1, k).wait_recv()


def run_begin(ident, slab, mix, rows, parts):
    seqs, cores = lax.axis_size("seq"), lax.axis_size("tensor")
    share, width = rows.shape
    chunk = min(64, share)
    chunks = share // chunk
    sem = pltpu.SemaphoreType.DMA
    return pl.pallas_call(
        functools.partial(begin_kernel, (seqs, cores, share, chunk)),
        out_shape=(
            jax.ShapeDtypeStruct((parts,) + slab.shape, BF16),
            jax.ShapeDtypeStruct((parts,) + mix.shape, BF16),
            jax.ShapeDtypeStruct((seqs * cores * share, width), BF16),
        ),
        in_specs=[VMEM_SPEC] * 3,
        out_specs=[VMEM_SPEC] * 3,
        scratch_shapes=[
            sem((2, seqs - 1)), sem((2, seqs - 1)), sem((2, seqs, 2)), sem((2, seqs, 2)),
            sem((2, seqs)), sem((2, seqs)), sem((2, seqs, chunks)), sem((2, seqs, chunks)),
            sem((2, seqs, chunks, cores - 1)), sem((2, seqs, chunks, cores - 1)), sem((3,)),
        ],
        compiler_params=pltpu.CompilerParams(
            vmem_limit_bytes=56 * 1024 * 1024, collective_id=ident, has_side_effects=True
        ),
        name="begin",
    )(slab, mix, rows)


def conv_silu(padded, kernel):
    row_count = padded.shape[0] - K + 1
    running = kernel[K]
    for offset in range(K):
        running = running + kernel[offset] * padded[offset : offset + row_count]
    return jax.nn.silu(running)


def prenorm(residual, gain_pre):
    return (
        residual
        * lax.rsqrt(jnp.mean(residual * residual, axis=-1, keepdims=True) + EPSILON)
        * gain_pre
    )


def pad_to(value, rows, columns):
    return jnp.pad(value, ((0, rows - value.shape[0]), (0, columns - value.shape[1])))


def body(
    hidden, lengths, pre_gain, w_zx, w_bc, w_dt, conv_x, conv_bc, head_params,
    norm_gain, w_out, cotangent,
):
    seqs, cores, parts = (lax.axis_size(a) for a in ("seq", "tensor", "dp"))
    place, core = lax.axis_index("seq"), lax.axis_index("tensor")
    piece, width = hidden.shape[1], hidden.shape[2]
    tokens, share = piece * seqs, piece // cores
    depth = w_zx.shape[1]
    inner = w_zx.shape[3] // seqs
    heads = w_dt.shape[2] // seqs
    pair_cols = w_bc.shape[2]
    bc_at = 2 * inner
    step_at = bc_at + -(-pair_cols // LANES) * LANES
    slab_cols = step_at + LANES
    sizes = (tokens, inner, heads, step_at)
    live = (jnp.arange(tokens, dtype=jnp.int32) < lengths[0]).astype(F32)[:, None]

    def own_rows(value):
        return lax.dynamic_slice_in_dim(value[0], core * share, share, 0)

    slabs, mixes = [], []
    for layer in range(L):
        wide = w_zx[layer].reshape(depth, 2, seqs, inner).transpose(2, 0, 1, 3)
        wide = wide.reshape(seqs, depth, 2 * inner)
        pair_part = jnp.broadcast_to(w_bc[layer][None], (seqs, depth, pair_cols))
        pair_part = jnp.pad(pair_part, ((0, 0), (0, 0), (0, step_at - bc_at - pair_cols)))
        step_part = w_dt[layer].reshape(depth, seqs, heads).transpose(1, 0, 2)
        step_part = jnp.pad(step_part, ((0, 0), (0, 0), (0, LANES - heads)))
        slab = jnp.concatenate([wide, pair_part, step_part], axis=2)
        mix = w_out[layer].reshape(seqs, inner, depth)
        if layer == 0:
            slab, mix, hidden_full = run_begin(2 * L, slab, mix, own_rows(hidden), parts)
            gate = hidden_full
        else:
            slab, mix, gate = lax.optimization_barrier((slab, mix, gate))
            slab = gather_axis(exchange_axis(slab, "seq"), "dp")
            mix = gather_axis(exchange_axis(mix, "seq"), "dp")
        slabs.append(slab.reshape(width, slab_cols))
        mixes.append(mix.reshape(parts * seqs, inner, depth))

    def end_rows(value):
        upper = place >= seqs // 2
        shaped = value.reshape(2, seqs // 2, cores, share, width)
        mine = pick(jnp.moveaxis(pick(shaped, upper.astype(jnp.int32)), 1, 0), core)
        return jnp.where(upper, mine, mine[::-1]).reshape(seqs // 2 * share, width)

    cotangent, gate = lax.optimization_barrier((cotangent, gate))
    upstream_full = gather_rows(own_rows(cotangent))
    residual = end_rows(hidden_full).astype(F32)
    upstream = end_rows(upstream_full)
    normed = prenorm(hidden_full.astype(F32), pre_gain[0]).astype(BF16)

    def tensor_columns(value):
        if cores == 2:
            other = swap(value, "tensor", 1)
            first = jnp.where(core == 0, value, other)
            return jnp.concatenate([first, jnp.where(core == 0, other, value)], axis=1)
        parts_of = gather_axis(value, "tensor")
        return jnp.moveaxis(parts_of, 0, 1).reshape(value.shape[0], -1)

    kept = []
    for layer in range(L):
        conv = pad_to(
            lax.dynamic_slice_in_dim(conv_x[layer], place * inner, inner, 1), 8, inner
        )
        head_rows = pad_to(
            lax.dynamic_slice_in_dim(head_params[layer], place * heads, heads, 1), 8, LANES
        )
        gain = lax.dynamic_slice_in_dim(norm_gain[layer], place * inner, inner, 0)[None]
        entry = residual
        proj = jnp.dot(normed, slabs[layer], preferred_element_type=F32)
        pair_raw = (proj[:, bc_at : bc_at + pair_cols] * live).astype(BF16)
        padded_pair = jnp.pad(pair_raw.astype(F32), ((K - 1, 0), (0, 0)))
        pairs = tensor_columns(conv_silu(padded_pair, conv_bc[layer]).astype(BF16))
        outputs, mixed, inputs, states, squares = run_forward(
            sizes, lengths, proj, pairs, conv, head_rows, gain
        )
        if layer + 1 < L:
            full, residual, raw = run_reduce(
                "forward_middle", layer, mixed, mixes[layer], pre_gain[layer + 1][None],
                (squares, residual),
            )
            extra = full[:, width:]
        else:
            extra, result_low = run_reduce(
                "forward_last", layer, mixed, mixes[layer], pre_gain[layer][None],
                (squares, residual, upstream),
            )
            raw, up_extra = None, extra
        kept.append(
            (entry, raw, normed, proj, padded_pair, pairs, outputs, inputs, states, extra,
             conv, head_rows, gain)
        )
        if layer + 1 < L:
            normed = full[:, :width]

    shared, owned, pair_convs = [None] * L, [None] * L, [None] * L
    slab_grads, mix_grads = [None] * L, [None] * L
    for layer in reversed(range(L)):
        (entry, raw, normed, proj, padded_pair, pairs, outputs, inputs, states, extra,
         conv, head_rows, gain) = kept[layer]
        mixed_in, slab, bc, conv_grad, head_grad, small = run_backward(
            sizes, lengths, proj, pairs, conv, head_rows, gain, inputs, outputs, states,
            upstream_full, mixes[layer], extra, up_extra,
        )
        mix_grad = lax.dot_general(
            mixed_in, upstream_full[:, :width], (TN, ((), ())), preferred_element_type=F32
        )
        bc = jnp.moveaxis(bc.reshape(tokens, cores, pair_cols), 1, 0)
        bc = sum_axis(scatter_axis(bc, "tensor", F32), "seq", BF16)
        unused, pull_pair = jax.vjp(conv_silu, padded_pair, conv_bc[layer])
        d_padded, d_conv_bc = pull_pair(bc)
        d_pair = (d_padded[K - 1 :] * live).astype(BF16)
        slab = lax.dynamic_update_slice_in_dim(
            slab, pad_to(d_pair / seqs, tokens, step_at - bc_at), bc_at, 1
        )
        if layer > 0:
            upstream_full, d_pre, upstream = run_reduce(
                "backward_middle", L + layer, slab, slabs[layer], pre_gain[layer][None],
                (entry, upstream, kept[layer - 1][1]),
            )
            up_extra = upstream_full[:, width:]
        else:
            d_own, d_pre = run_reduce(
                "backward_last", L + layer, slab, slabs[layer], pre_gain[layer][None],
                (entry, upstream),
            )
        slab_grad = lax.dot_general(normed, slab, (TN, ((), ())), preferred_element_type=F32)
        slab_grad = scatter_axis(slab_grad.reshape(parts, seqs, depth, slab_cols), "dp")
        slab_grads[layer] = exchange_axis(slab_grad.astype(BF16), "seq").astype(F32)
        mix_grad = mix_grad.reshape(inner, parts, seqs, depth).transpose(1, 2, 0, 3)
        mix_grad = scatter_axis(mix_grad, "dp")
        mix_grads[layer] = exchange_axis(mix_grad.astype(BF16), "seq").astype(F32)
        skip = small[1].reshape(heads, P_SIZE).sum(-1)
        shared[layer] = d_pre[0]
        pair_convs[layer] = d_conv_bc
        owned[layer] = jnp.concatenate(
            [conv_grad[: K + 1].reshape(-1), small[0], head_grad[:2, :heads].reshape(-1), skip]
        )

    result = gather_axis(result_low, "tensor").reshape(piece, width)
    d_hidden = gather_axis(d_own, "tensor").reshape(piece, width)
    d_pre = jnp.stack(shared)
    for axis in ("dp", "seq", "tensor"):
        d_pre = sum_axis(d_pre, axis)
    small_sums = sum_axis(jnp.stack(owned), "dp")
    small_all = jnp.moveaxis(gather_axis(small_sums, "seq"), 0, 1)
    pair_sums = sum_axis(jnp.stack(pair_convs), "dp")

    def columns(first, count, each):
        part = small_all[:, :, first : first + count * each].reshape(L, seqs, count, each)
        return part.transpose(0, 2, 1, 3).reshape(L, count, seqs * each)

    edge = (K + 1) * inner
    slab_all = jnp.stack(slab_grads)
    d_zx = slab_all[..., :bc_at].reshape(L, seqs, depth, 2, inner).transpose(0, 2, 3, 1, 4)
    d_bc = slab_all[..., bc_at : bc_at + pair_cols].sum(1)
    d_dt = slab_all[..., step_at : step_at + heads].transpose(0, 2, 1, 3)
    return (
        result[None],
        d_hidden[None],
        d_pre,
        d_zx.reshape(L, depth, 2, seqs * inner),
        d_bc,
        d_dt.reshape(L, depth, seqs * heads),
        columns(0, K + 1, inner),
        pair_sums,
        columns(edge + inner, 3, heads),
        columns(edge, 1, inner)[:, 0],
        jnp.stack(mix_grads).reshape(L, seqs * inner, depth),
    )


def solution(mesh):
    wide = P(None, ("dp", "seq"), None, "tensor")
    thin = P(None, ("dp", "seq"), "tensor")
    rows = P("dp", "seq", None)
    flat = P(None, None, "tensor")
    gain = P(None, "tensor")
    mix = P(None, "tensor", ("dp", "seq"))
    return jax.shard_map(
        body,
        mesh=mesh,
        in_specs=(rows, P("dp"), P(), wide, thin, thin, flat, flat, flat, gain, mix, rows),
        out_specs=(rows, rows, P(), wide, thin, thin, flat, flat, flat, gain, mix),
        check_vma=False,
    )
```

```python
import functools

import jax
import jax.numpy as jnp
from jax import lax
from jax.experimental import pallas as pl
from jax.experimental.pallas import tpu as pltpu
from jax.sharding import PartitionSpec as P

DI = 4096
P_SIZE = 64
N = 128
K = 4
Q = 256
L = 2
LANES = 128
EPSILON = 1e-05
CHUNK = 32
LAG = 2
F32 = jnp.float32
BF16 = jnp.bfloat16
PRECISE = lax.Precision.HIGHEST


def swap(value, axis, distance):
    size = lax.axis_size(axis)
    return lax.ppermute(value, axis, [(i, i ^ distance) for i in range(size)])


def pick(value, index):
    return lax.dynamic_index_in_dim(value, index, 0, False)


def put(buffer, value, index):
    return lax.dynamic_update_index_in_dim(buffer, value, index, 0)


def gather_axis(value, axis):
    size, place = lax.axis_size(axis), lax.axis_index(axis)
    out = put(jnp.zeros((size,) + value.shape, value.dtype), value, place)
    for distance in range(1, size):
        out = put(out, swap(value, axis, distance), place ^ distance)
    return out


def exchange_axis(values, axis):
    size, place = lax.axis_size(axis), lax.axis_index(axis)
    out = put(jnp.zeros_like(values), pick(values, place), place)
    for distance in range(1, size):
        out = put(out, swap(pick(values, place ^ distance), axis, distance), place ^ distance)
    return out


def scatter_axis(values, axis, kind=BF16):
    size, place = lax.axis_size(axis), lax.axis_index(axis)
    total = pick(values, place).astype(F32)
    for distance in range(1, size):
        sent = pick(values, place ^ distance).astype(kind)
        total = total + swap(sent, axis, distance).astype(F32)
    return total


def sum_axis(value, axis, kind=F32):
    size = lax.axis_size(axis)
    distance = 1
    while distance < size:
        value = value + swap(value.astype(kind), axis, distance).astype(value.dtype)
        distance *= 2
    return value


def gather_rows(own):
    along = gather_axis(own, "seq")
    both = jnp.swapaxes(gather_axis(along, "tensor"), 0, 1)
    return both.reshape((-1,) + own.shape[1:])


def scatter_rows(partial):
    seqs, cores = lax.axis_size("seq"), lax.axis_size("tensor")
    parts = partial.reshape((seqs, cores, -1) + partial.shape[1:])
    halves = scatter_axis(jnp.swapaxes(parts, 0, 1), "tensor")
    return scatter_axis(halves, "seq")


def lane_iota(shape):
    return lax.broadcasted_iota(jnp.int32, shape, len(shape) - 1)


def row_iota(shape):
    return lax.broadcasted_iota(jnp.int32, shape, len(shape) - 2)


def dot(a, b, dims, precision=None):
    return lax.dot_general(
        a, b, (dims, ((), ())), preferred_element_type=F32, precision=precision
    )


NN = ((1,), (0,))
NT = ((1,), (1,))
TN = ((0,), (0,))


def pair_of(columns, j):
    rows = columns.shape[0]
    first = lane_iota((rows, LANES)) < P_SIZE
    return jnp.where(first, columns[:, 2 * j : 2 * j + 1], columns[:, 2 * j + 1 : 2 * j + 2])


def spread(columns, heads):
    return jnp.concatenate([pair_of(columns, j) for j in range(heads // 2)], axis=1)


def split_pair(pair):
    first = lane_iota(pair.shape) < P_SIZE
    zero = jnp.zeros_like(pair)
    return jnp.where(first, pair, zero), jnp.where(first, zero, pair)


def block_steps(raw, head_rows, live):
    steps = jax.nn.softplus(raw + head_rows[1:2]) * live
    rate = -jnp.exp(head_rows[0:1])
    return steps, rate


def sigmoid(v):
    return 1.0 / (1.0 + jnp.exp(-v))


def forward_kernel(
    sizes, length_ref, proj_ref, pairs_ref, conv_ref, head_ref, gain_ref,
    outputs_ref, mixed_ref, inputs_ref, states_ref, square_ref, state, halo,
):
    tokens, inner, heads, step_at = sizes
    head_rows = head_ref[...]
    head_lane = lane_iota((1, LANES)) < heads
    causal = row_iota((Q, Q)) >= lane_iota((Q, Q))
    below = causal.astype(F32)
    state[...] = jnp.zeros_like(state)
    halo[...] = jnp.zeros_like(halo)
    length = length_ref[0]

    def block(k, carry):
        start = pl.multiple_of(k * Q, Q)
        rows = pl.ds(start, Q)
        live = (row_iota((Q, 1)) + start < length).astype(F32)
        raw = (proj_ref[rows, inner : 2 * inner].astype(F32) * live).astype(BF16).astype(F32)
        padded = jnp.concatenate([halo[...], raw], axis=0)
        halo[...] = raw[Q - 8 :]
        pre = conv_ref[K : K + 1, :]
        for tap in range(K):
            pre = pre + conv_ref[tap : tap + 1, :] * padded[5 + tap : 5 + tap + Q]
        inputs = (pre * sigmoid(pre)).astype(BF16)
        inputs_ref[rows, :] = inputs
        steps, rate = block_steps(proj_ref[rows, step_at : step_at + LANES], head_rows, live)
        decay = jnp.where(head_lane, steps * rate, 0.0)
        cum = dot(below, decay, NN, PRECISE)
        cum_t = cum.T
        b_rows = pairs_ref[rows, :N]
        c_rows = pairs_ref[rows, N:]
        scores = jnp.where(causal, dot(c_rows, b_rows, NT), 0.0)
        before = state[...]
        states_ref[k] = before
        inputs_f = inputs.astype(F32)
        scaled = inputs_f * spread(steps, heads)
        scaled_low = scaled.astype(BF16)
        across = dot(c_rows, before.astype(BF16), NT) * spread(jnp.exp(cum), heads)
        last = cum[Q - 1 : Q]
        tail = jnp.exp(last - cum)
        square = jnp.zeros((Q, 1), F32)
        for j in range(heads // 2):
            cols = slice(j * LANES, (j + 1) * LANES)
            mixing = []
            for h in (2 * j, 2 * j + 1):
                gap = jnp.minimum(cum[:, h : h + 1] - cum_t[h : h + 1, :], 0.0)
                mixing.append((jnp.exp(gap) * scores).astype(BF16))
            both = jnp.concatenate(mixing, axis=1)
            stacked = jnp.concatenate(split_pair(scaled_low[:, cols]), axis=0)
            out = dot(both, stacked, NN) + across[:, cols]
            out = out + pair_of(head_rows[2:3], j) * inputs_f[:, cols]
            outputs_ref[rows, cols] = out
            gate = proj_ref[rows, cols]
            gated = out * gate * sigmoid(gate)
            mixed_ref[rows, cols] = (gated * gain_ref[:, cols]).astype(BF16)
            square = square + jnp.sum(gated * gated, axis=1, keepdims=True)
        square_ref[rows, :] = jnp.broadcast_to(square, (Q, LANES))
        fresh = dot((scaled * spread(tail, heads)).astype(BF16), b_rows, TN)
        for h in range(heads):
            own = slice(h * P_SIZE, (h + 1) * P_SIZE)
            state[own, :] = jnp.exp(last[:, h : h + 1]) * before[own] + fresh[own]
        return carry

    lax.fori_loop(0, tokens // Q, block, 0)


def backward_kernel(
    sizes, length_ref, proj_ref, pairs_ref, conv_ref, head_ref, gain_ref, inputs_ref,
    outputs_ref, states_ref, up_ref, mix_ref, extra_ref, up_extra_ref,
    mixed_ref, slab_ref, bc_ref, conv_grad_ref, head_grad_ref, small_ref, state, halo,
    scratch_a, scratch_b, scratch_c, mixgrad_ref,
):
    tokens, inner, heads, step_at = sizes
    head_rows = head_ref[...]
    head_lane = lane_iota((1, LANES)) < heads
    causal = row_iota((Q, Q)) >= lane_iota((Q, Q))
    below = causal.astype(F32)
    onehot = (row_iota((inner, LANES)) // P_SIZE == lane_iota((inner, LANES))).astype(F32)
    state[...] = jnp.zeros_like(state)
    halo[...] = jnp.zeros_like(halo)
    conv_grad_ref[...] = jnp.zeros_like(conv_grad_ref)
    head_grad_ref[...] = jnp.zeros_like(head_grad_ref)
    small_ref[...] = jnp.zeros_like(small_ref)
    length = length_ref[0]
    blocks = tokens // Q

    def block(turn, carry):
        k = blocks - 1 - turn
        start = pl.multiple_of(k * Q, Q)
        rows = pl.ds(start, Q)
        live = (row_iota((Q, 1)) + start < length).astype(F32)
        steps, rate = block_steps(proj_ref[rows, step_at : step_at + LANES], head_rows, live)
        decay = jnp.where(head_lane, steps * rate, 0.0)
        cum = dot(below, decay, NN, PRECISE)
        cum_t = cum.T
        last = cum[Q - 1 : Q]
        grow = jnp.exp(cum)
        tail = jnp.exp(last - cum)
        b_rows = pairs_ref[rows, :N]
        c_rows = pairs_ref[rows, N:]
        scores = jnp.where(causal, dot(c_rows, b_rows, NT), 0.0)
        before = states_ref[k]
        before_low = before.astype(BF16)
        after = state[...]
        after_low = after.astype(BF16)
        scale = joined(extra_ref[rows, :], 0, 3)
        coef = scale * scale * scale * joined(up_extra_ref[rows, :], 3, 2) / DI
        mixgrad = jnp.zeros((Q, inner), F32)
        for n in range(mix_ref.shape[0] // 512):
            part = slice(n * 512, (n + 1) * 512)
            mixgrad = mixgrad + dot(up_ref[rows, part], mix_ref[part, :inner], NN)
        mixgrad_ref[...] = mixgrad
        spread_b = dot(b_rows, after_low, NT)
        pair_sum = jnp.zeros((Q, Q), F32)
        for j in range(heads // 2):
            cols = slice(j * LANES, (j + 1) * LANES)
            steps_j, grow_j, tail_j = pair_of(steps, j), pair_of(grow, j), pair_of(tail, j)
            skip_j = pair_of(head_rows[2:3], j)
            gate = proj_ref[rows, cols]
            sig = sigmoid(gate)
            silu = gate * sig
            out = outputs_ref[rows, cols]
            gated = out * silu
            mixgrad = mixgrad_ref[:, cols]
            gain = gain_ref[:, cols]
            normal = gated * scale
            small_ref[0:1, cols] += jnp.sum(mixgrad * normal, axis=0, keepdims=True)
            mixed_ref[rows, cols] = (normal * gain).astype(BF16)
            d_gated = scale * (mixgrad * gain) - gated * coef
            d_out = d_gated * silu
            slab_ref[rows, cols] = (
                d_gated * out * sig * (1.0 + gate * (1.0 - sig))
            ).astype(BF16)
            d_low = d_out.astype(BF16)
            inputs = inputs_ref[rows, cols].astype(F32)
            small_ref[1:2, cols] += jnp.sum(d_out * inputs, axis=0, keepdims=True)
            scaled = inputs * steps_j
            scaled_low = scaled.astype(BF16)
            d_halves = split_pair(d_low)
            mixing = []
            for at, h in enumerate((2 * j, 2 * j + 1)):
                gap = jnp.minimum(cum[:, h : h + 1] - cum_t[h : h + 1, :], 0.0)
                fade = jnp.exp(gap)
                mixing.append((fade * scores).astype(BF16))
                pair_sum = pair_sum + fade * dot(d_halves[at], scaled_low, NT)
            y_tail = spread_b[:, cols] * tail_j
            y = dot(jnp.concatenate(mixing, axis=0), jnp.concatenate(d_halves, axis=0), TN)
            y = y + y_tail
            scaled_f = scaled_low.astype(F32)
            scratch_a[:, cols] = inputs * y
            scratch_b[:, cols] = d_low.astype(F32) * (out - skip_j * inputs) - scaled_f * y
            small_ref[2:3, cols] = jnp.sum(scaled_f * y_tail, axis=0, keepdims=True)
            scratch_c[:, cols] = steps_j * y + skip_j * d_out
            mixed_low = (d_out * grow_j).astype(BF16)
            slab_ref[rows, inner + j * LANES : inner + (j + 1) * LANES] = mixed_low
        grown = slab_ref[rows, inner : 2 * inner]
        pair_low = jnp.where(causal, pair_sum, 0.0).astype(BF16)
        tailed = (inputs_ref[rows, :].astype(F32) * spread(steps * tail, heads)).astype(BF16)
        bc_ref[rows, :N] = dot(pair_low, c_rows, TN) + dot(tailed, after_low, NN)
        bc_ref[rows, N:] = dot(pair_low, b_rows, NN) + dot(grown, before_low, NN)
        kept = dot(jnp.ones((8, N), F32), after_low.astype(F32) * before, NT, PRECISE)
        ends = dot(kept, onehot, NN, PRECISE)[0:1] * jnp.exp(last)
        ends = ends + dot(
            jnp.broadcast_to(small_ref[2:3, :], (8, inner)), onehot, NN, PRECISE
        )[0:1]
        d_decay = dot(below, dot(scratch_b[...], onehot, NN, PRECISE), TN, PRECISE) + ends
        d_steps = dot(scratch_a[...], onehot, NN, PRECISE) + rate * d_decay
        d_soft = d_steps * live * sigmoid(
            proj_ref[rows, step_at : step_at + LANES] + head_rows[1:2]
        )
        d_soft = jnp.where(head_lane, d_soft, 0.0)
        slab_ref[rows, step_at : step_at + LANES] = d_soft.astype(BF16)
        head_grad_ref[0:1, :] += rate * jnp.sum(
            jnp.where(head_lane, steps * d_decay, 0.0), axis=0, keepdims=True
        )
        head_grad_ref[1:2, :] += jnp.sum(d_soft, axis=0, keepdims=True)
        gathered = dot(grown, c_rows, TN)
        for h in range(heads):
            own = slice(h * P_SIZE, (h + 1) * P_SIZE)
            state[own, :] = jnp.exp(last[:, h : h + 1]) * after[own] + gathered[own]
        raw = (proj_ref[rows, inner : 2 * inner] * live).astype(BF16).astype(F32)
        ahead = pl.ds(pl.multiple_of(jnp.maximum(start - 8, 0), 8), 8)
        earlier = row_iota((8, 1)) + start - 8
        ahead_live = jnp.logical_and(earlier >= 0, earlier < length).astype(F32)
        first = (proj_ref[ahead, inner : 2 * inner] * ahead_live).astype(BF16).astype(F32)
        padded = jnp.concatenate([first, raw], axis=0)
        pre = conv_ref[K : K + 1, :]
        for tap in range(K):
            pre = pre + conv_ref[tap : tap + 1, :] * padded[5 + tap : 5 + tap + Q]
        sig = sigmoid(pre)
        d_pre = scratch_c[...] * sig * (1.0 + pre * (1.0 - sig))
        after_pre = jnp.concatenate([d_pre, halo[...]], axis=0)
        halo[...] = d_pre[0:8]
        d_raw = jnp.zeros((Q, inner), F32)
        for tap in range(K):
            conv_grad_ref[tap : tap + 1, :] += jnp.sum(
                d_pre * padded[5 + tap : 5 + tap + Q], axis=0, keepdims=True
            )
            d_raw = d_raw + conv_ref[tap : tap + 1, :] * after_pre[3 - tap : 3 - tap + Q]
        conv_grad_ref[K : K + 1, :] += jnp.sum(d_pre, axis=0, keepdims=True)
        slab_ref[rows, inner : 2 * inner] = (d_raw * live).astype(BF16)
        return carry

    lax.fori_loop(0, blocks, block, 0)


VMEM_SPEC = pl.BlockSpec(memory_space=pltpu.VMEM)
SMEM_SPEC = pl.BlockSpec(memory_space=pltpu.SMEM)

PARAMS = pltpu.CompilerParams(vmem_limit_bytes=56 * 1024 * 1024)


def run_forward(sizes, lengths, proj, pairs, conv, heads_in, gain):
    tokens, inner, heads, step_at = sizes
    shapes = (
        jax.ShapeDtypeStruct((tokens, inner), F32),
        jax.ShapeDtypeStruct((tokens, inner), BF16),
        jax.ShapeDtypeStruct((tokens, inner), BF16),
        jax.ShapeDtypeStruct((tokens // Q, inner, N), F32),
        jax.ShapeDtypeStruct((tokens, LANES), F32),
    )
    return pl.pallas_call(
        functools.partial(forward_kernel, sizes),
        out_shape=shapes,
        in_specs=[SMEM_SPEC] + [VMEM_SPEC] * 5,
        out_specs=[VMEM_SPEC] * 5,
        scratch_shapes=[pltpu.VMEM((inner, N), F32), pltpu.VMEM((8, inner), F32)],
        compiler_params=PARAMS,
        cost_estimate=pl.CostEstimate(flops=8 * 10**9, bytes_accessed=16 * 10**6, transcendentals=4 * 10**6),
        name="scan_forward",
    )(lengths, proj, pairs, conv, heads_in, gain)


def run_backward(sizes, lengths, proj, pairs, conv, heads_in, gain, inputs, outputs, states, up, mix, extra, up_extra):
    tokens, inner, heads, step_at = sizes
    width = proj.shape[1]
    shapes = (
        jax.ShapeDtypeStruct((tokens, inner), BF16),
        jax.ShapeDtypeStruct((tokens, width), BF16),
        jax.ShapeDtypeStruct((tokens, 2 * N), F32),
        jax.ShapeDtypeStruct((8, inner), F32),
        jax.ShapeDtypeStruct((8, LANES), F32),
        jax.ShapeDtypeStruct((8, inner), F32),
    )
    return pl.pallas_call(
        functools.partial(backward_kernel, sizes),
        out_shape=shapes,
        in_specs=[SMEM_SPEC] + [VMEM_SPEC] * 12,
        out_specs=[VMEM_SPEC] * 6,
        scratch_shapes=[
            pltpu.VMEM((inner, N), F32),
            pltpu.VMEM((8, inner), F32),
        ]
        + [pltpu.VMEM((Q, inner), F32)] * 4,
        compiler_params=PARAMS,
        cost_estimate=pl.CostEstimate(flops=20 * 10**9, bytes_accessed=24 * 10**6, transcendentals=6 * 10**6),
        name="scan_backward",
    )(lengths, proj, pairs, conv, heads_in, gain, inputs, outputs, states, up, mix, extra, up_extra)


def joined(extra, first, count):
    total = extra[:, first : first + 1].astype(F32)
    for lane in range(first + 1, first + count):
        total = total + extra[:, lane : lane + 1].astype(F32)
    return total


def parted(columns):
    rows = columns[0][0].shape[0]
    lane = lane_iota((rows, LANES))
    out = jnp.zeros((rows, LANES), F32)
    for value, first, count in columns:
        rest = value
        for at in range(count):
            part = rest.astype(BF16).astype(F32)
            out = jnp.where(lane == first + at, part, out)
            rest = rest - part
    return out.astype(BF16)


def reduce_kernel(mode, dims, *refs):
    seqs, cores, tokens, width, share, chunk = dims
    forward, last = mode.startswith("forward"), mode.endswith("last")
    refs = list(refs)
    take = lambda count: [refs.pop(0) for _ in range(count)]
    lhs_ref, rhs_ref, gain_ref = take(3)
    depth = lhs_ref.shape[1]
    skipped = 0 if forward else rhs_ref.shape[1] - depth
    if forward:
        square_ref, res_ref = take(2)
        up_ref = take(1)[0] if last else None
    else:
        res_ref, up_ref = take(2)
        raw_ref = None if last else take(1)[0]
    bulk = mode != "forward_last"
    if bulk:
        bulk_in = take(1)[0]
    full_ref = None if mode == "backward_last" else take(1)[0]
    if last:
        own_ref = take(1)[0]
    if forward:
        if not last:
            new_ref, raw_out = take(2)
    else:
        gain_out = take(1)[0]
        if not last:
            new_ref = take(1)[0]
    if bulk:
        bulk_out = take(1)[0]
        if mode == "backward_last":
            bulk_end = take(1)[0]
    stage, core_recv, send, recv = take(4)
    if last:
        hold = take(1)[0]
    if bulk and not forward:
        bulk_one, bulk_two = take(2)
    core_ss, core_rs, ss, rs, ag_ss, ag_rs, sib_ss, sib_rs, own_ss, own_rs = take(10)
    if bulk:
        bulk_ss, bulk_rs, far_ss, far_rs = take(4)
        part = lax.axis_index("dp")
        near = {1: part + 1 - 2 * lax.rem(part, 2), 2: lax.rem(part + 2, 4)}
    if mode == "backward_last":
        end_ss, end_rs = take(2)

    place, core = lax.axis_index("seq"), lax.axis_index("tensor")
    half, piece, pieces = tokens // 2, share * cores, seqs // 2
    rows_own = share * pieces
    per_piece = share // chunk
    chunks = rows_own // chunk
    pos = {1: place, 0: seqs - 1 - place}
    step = {1: 1, 0: -1}
    mesh_id = pl.DeviceIdType.MESH

    barrier = pltpu.get_barrier_semaphore()
    peers = [{"dp": near[1]}, {"dp": near[2]}] if bulk else []
    for a in range(seqs):
        for b in range(cores):
            if a or b:
                peers.append(
                    {"seq": lax.rem(place + a, seqs), "tensor": lax.rem(core + b, cores)}
                )
    for peer in peers:
        pl.semaphore_signal(barrier, inc=1, device_id=peer, device_id_type=mesh_id)
    pl.semaphore_wait(barrier, len(peers))

    def remote(source, target, send_sem, recv_sem, device):
        return pltpu.make_async_remote_copy(
            src_ref=source, dst_ref=target, send_sem=send_sem, recv_sem=recv_sem,
            device_id=device, device_id_type=mesh_id,
        )

    if bulk and forward:

        def bulk_near(s, bit):
            return remote(
                bulk_in.at[s], bulk_out.at[part, s], bulk_ss.at[s, bit - 1],
                bulk_rs.at[s, bit - 1], {"dp": near[bit]},
            )

        def bulk_far(s):
            target = bulk_out.at[near[1 + s % 2], s]
            return remote(target, target, far_ss.at[s], far_rs.at[s], {"dp": near[2 - s % 2]})

        for s in range(seqs):
            for bit in (1, 2):
                bulk_near(s, bit).start()
        bulk_out[part] = bulk_in[...]
    elif bulk:

        def bulk_first(s, at):
            bit = 1 + s % 2
            of = near[bit] if at == 0 else 3 - part
            return remote(
                bulk_in.at[of, s], bulk_one.at[s, at], bulk_ss.at[s, at], bulk_rs.at[s, at],
                {"dp": near[bit]},
            )

        def bulk_second(s):
            return remote(
                bulk_one.at[s, 1], bulk_two.at[s], far_ss.at[s], far_rs.at[s],
                {"dp": near[2 - s % 2]},
            )

        for at in (1, 0):
            for s in range(seqs):
                bulk_first(s, at).start()

    def bulk_middle():
        for s in range(seqs):
            if forward:
                for bit in (1, 2):
                    bulk_near(s, bit).wait_recv()
                bulk_far(s).start()
            else:
                bulk_first(s, 1).wait()
                total = bulk_one[s, 1].astype(F32) + bulk_in[near[2 - s % 2], s].astype(F32)
                bulk_one[s, 1] = total.astype(BF16)
                bulk_second(s).start()

    def bulk_last():
        for s in range(seqs):
            if forward:
                for bit in (1, 2):
                    bulk_near(s, bit).wait_send()
                bulk_far(s).wait()
            else:
                bulk_first(s, 0).wait()
                bulk_second(s).wait()
                total = bulk_one[s, 0].astype(F32) + bulk_in[part, s].astype(F32)
                bulk_out[s] = (total + bulk_two[s].astype(F32)).astype(BF16)
        if mode == "backward_last":

            def end(o):
                to = lax.rem(place + o, seqs)
                return remote(
                    bulk_out.at[to], bulk_end.at[place], end_ss.at[o - 1], end_rs.at[o - 1],
                    {"seq": to},
                )

            for o in range(1, seqs):
                end(o).start()
            bulk_end[place] = bulk_out[place]
            for o in range(1, seqs):
                end(o).wait()

    def piece_at(direction, p):
        return p if direction else pieces - 1 - p

    def start_of(direction, at_core, j):
        p, inside = j // per_piece, lax.rem(j, per_piece)
        base = direction * half + piece_at(direction, p) * piece
        return pl.multiple_of(base + at_core * share + inside * chunk, chunk)

    tile = 256
    for direction in (1, 0):
        lhs_rows = slice(direction * half, (direction + 1) * half)

        def columns(n, carry):
            at = pl.ds(pl.multiple_of(n * tile, tile), tile)
            lhs = lhs_ref[lhs_rows, :]
            value = dot(lhs, rhs_ref[at, skipped : skipped + depth], NT).astype(BF16)
            for p in range(pieces):
                for b in range(cores):
                    first = piece_at(direction, p) * piece + b * share
                    stage[b, direction, p * share : (p + 1) * share, at] = value[
                        first : first + share
                    ]
            return carry

        lax.fori_loop(0, width // tile, columns, 0)
        if forward:
            for p in range(pieces):
                for b in range(cores):
                    first = direction * half + piece_at(direction, p) * piece + b * share
                    stage[b, direction, p * share : (p + 1) * share, width:] = parted(
                        [(square_ref[first : first + share, 0:1], 0, 2)]
                    )
        for o in range(1, cores):
            core_copy(stage, core_recv, core_ss, core_rs, core, cores, o, direction).start()

    def chain_copy(direction, j):
        rows = pl.ds(pl.multiple_of(j * chunk, chunk), chunk)
        return pltpu.make_async_remote_copy(
            src_ref=send.at[direction, rows], dst_ref=recv.at[direction, rows],
            send_sem=ss.at[direction, j], recv_sem=rs.at[direction, j],
            device_id={"seq": place + step[direction]}, device_id_type=mesh_id,
        )

    def back_copy(direction, j):
        rows = pl.ds(start_of(direction, core, j), chunk)
        return pltpu.make_async_remote_copy(
            src_ref=full_ref.at[rows], dst_ref=full_ref.at[rows],
            send_sem=ag_ss.at[direction, j], recv_sem=ag_rs.at[direction, j],
            device_id={"seq": place - step[direction]}, device_id_type=mesh_id,
        )

    def side_copy(direction, j, o, at_core):
        rows = pl.ds(start_of(direction, at_core, j), chunk)
        return pltpu.make_async_remote_copy(
            src_ref=full_ref.at[rows], dst_ref=full_ref.at[rows],
            send_sem=sib_ss.at[o - 1, direction, j], recv_sem=sib_rs.at[o - 1, direction, j],
            device_id={"tensor": lax.rem(core + o, cores)}, device_id_type=mesh_id,
        )

    def own_copy(direction, j):
        inside = lax.rem(j, per_piece)
        rows = pl.ds(pl.multiple_of(j * chunk, chunk), chunk)
        to = direction * pieces + piece_at(direction, j // per_piece)
        return pltpu.make_async_remote_copy(
            src_ref=hold.at[rows],
            dst_ref=own_ref.at[pl.ds(pl.multiple_of(inside * chunk, chunk), chunk)],
            send_sem=own_ss.at[j], recv_sem=own_rs.at[inside],
            device_id={"seq": to}, device_id_type=mesh_id,
        )

    def spread_out(direction, j):
        back_copy(direction, j).start()
        for o in range(1, cores):
            side_copy(direction, j, o, core).start()

    if not forward:
        gain_out[...] = jnp.zeros_like(gain_out)

    def finish(direction, j, total):
        rows = pl.ds(pl.multiple_of(j * chunk, chunk), chunk)
        out_rows = pl.ds(start_of(direction, core, j), chunk)
        gain = gain_ref[...]
        residual = res_ref[rows, :]
        if forward:
            square = total[:, width : width + 1] + total[:, width + 1 : width + 2]
            scale = lax.rsqrt(square / DI + EPSILON)
            raw = total[:, :width]
            value = residual + raw * scale
            if last:
                along = jnp.sum(up_ref[rows, :].astype(F32) * raw, axis=1, keepdims=True)
                full_ref[out_rows, :] = parted([(scale, 0, 3), (along, 3, 2)])
                result = value.astype(BF16)
            else:
                new_ref[rows, :] = value
                raw_out[rows, :] = raw
                mean = jnp.sum(value * value, axis=1, keepdims=True) / width
                full_ref[out_rows, :width] = (value * lax.rsqrt(mean + EPSILON) * gain).astype(BF16)
                full_ref[out_rows, width:] = parted([(scale, 0, 3)])
        else:
            mean = jnp.sum(residual * residual, axis=1, keepdims=True) / width
            q = lax.rsqrt(mean + EPSILON)
            scaled = total * gain
            gain_out[0:1, :] += jnp.sum(total * residual * q, axis=0, keepdims=True)
            along = jnp.sum(scaled * residual, axis=1, keepdims=True) / width
            value = up_ref[rows, :].astype(F32) + q * scaled - residual * (q * q * q * along)
            if last:
                result = value
            else:
                new_ref[rows, :] = value
                low = value.astype(BF16)
                full_ref[out_rows, :width] = low
                along = jnp.sum(low.astype(F32) * raw_ref[rows, :], axis=1, keepdims=True)
                full_ref[out_rows, width:] = parted([(along, 3, 2)])
        if full_ref is not None:
            spread_out(direction, j)
        if last:
            to = direction * pieces + piece_at(direction, j // per_piece)
            inside = pl.ds(pl.multiple_of(lax.rem(j, per_piece) * chunk, chunk), chunk)

            @pl.when(to == place)
            def _():
                own_ref[inside, :] = result

            @pl.when(to != place)
            def _():
                hold[rows, :] = result
                own_copy(direction, j).start()

    for o in range(1, cores):
        for direction in (1, 0):
            core_copy(stage, core_recv, core_ss, core_rs, core, cores, o, direction).wait()

    def chain(turn, carry):
        for direction in (1, 0):
            j = turn - LAG * pos[direction]
            rows = pl.ds(pl.multiple_of(j * chunk, chunk), chunk)
            due = jnp.logical_and(j >= 0, j < chunks)

            def local():
                value = stage[core, direction, rows, :].astype(F32)
                for o in range(1, cores):
                    value = value + core_recv[o - 1, direction, rows, :].astype(F32)
                return value

            def joint():
                chain_copy(direction, j).wait_recv()
                return local() + recv[direction, rows, :].astype(F32)

            def pass_on(value):
                if forward:
                    square = value[:, width : width + 1] + value[:, width + 1 : width + 2]
                    send[direction, rows, :width] = value[:, :width].astype(BF16)
                    send[direction, rows, width:] = parted([(square, 0, 2)])
                else:
                    send[direction, rows, :] = value.astype(BF16)
                chain_copy(direction, j).start()

            @pl.when(jnp.logical_and(due, pos[direction] == 0))
            def _():
                pass_on(local())

            inside = jnp.logical_and(pos[direction] > 0, pos[direction] < seqs - 1)

            @pl.when(jnp.logical_and(due, inside))
            def _():
                pass_on(joint())

            @pl.when(jnp.logical_and(due, pos[direction] == seqs - 1))
            def _():
                finish(direction, j, joint())

        return carry

    lax.fori_loop(0, chunks + LAG * (seqs - 1), chain, 0)
    if bulk:
        bulk_middle()

    if full_ref is not None:

        def back(turn, carry):
            for direction in (1, 0):
                away = seqs - 1 - pos[direction]
                j = turn - LAG * (away - 1)
                due = jnp.logical_and(j >= 0, j < chunks)

                @pl.when(jnp.logical_and(due, away > 0))
                def _():
                    back_copy(direction, j).wait_recv()

                    @pl.when(pos[direction] > 0)
                    def _():
                        back_copy(direction, j).start()

                    for o in range(1, cores):
                        side_copy(direction, j, o, core).start()

            return carry

        lax.fori_loop(0, chunks + LAG * (seqs - 2), back, 0)

    def drain(j, carry):
        for direction in (1, 0):

            @pl.when(pos[direction] < seqs - 1)
            def _():
                chain_copy(direction, j).wait_send()

            if full_ref is not None:

                @pl.when(pos[direction] > 0)
                def _():
                    back_copy(direction, j).wait_send()

                for o in range(1, cores):
                    side_copy(direction, j, o, core).wait_send()
                    side_copy(direction, j, o, lax.rem(core - o + cores, cores)).wait_recv()
            if last:
                to = direction * pieces + piece_at(direction, j // per_piece)

                @pl.when(jnp.logical_and(pos[direction] == seqs - 1, to != place))
                def _():
                    own_copy(direction, j).wait_send()

        return carry

    lax.fori_loop(0, chunks, drain, 0)
    if last:

        @pl.when(jnp.logical_and(place > 0, place < seqs - 1))
        def _():
            def arrived(j, carry):
                own_copy(0, j).wait_recv()
                return carry

            lax.fori_loop(0, per_piece, arrived, 0)

    if bulk:
        bulk_last()


def core_copy(stage, core_recv, core_ss, core_rs, core, cores, o, direction):
    to = lax.rem(core + o, cores)
    return pltpu.make_async_remote_copy(
        src_ref=stage.at[to, direction], dst_ref=core_recv.at[o - 1, direction],
        send_sem=core_ss.at[o - 1, direction], recv_sem=core_rs.at[o - 1, direction],
        device_id={"tensor": to}, device_id_type=pl.DeviceIdType.MESH,
    )


def run_reduce(mode, ident, lhs, rhs, gain, more, bulk=None):
    forward, last = mode.startswith("forward"), mode.endswith("last")
    seqs, cores = lax.axis_size("seq"), lax.axis_size("tensor")
    tokens, width = lhs.shape[0], gain.shape[1]
    share = tokens // (seqs * cores)
    chunk = min(CHUNK, share)
    dims = (seqs, cores, tokens, width, share, chunk)
    rows_own = share * seqs // 2
    chunks = rows_own // chunk
    full_width = width + LANES
    shapes = []
    if mode != "backward_last":
        shapes.append(jax.ShapeDtypeStruct((tokens, LANES if last else full_width), BF16))
    if last:
        shapes.append(jax.ShapeDtypeStruct((share, width), BF16 if forward else F32))
    if forward and not last:
        shapes += [jax.ShapeDtypeStruct((rows_own, width), F32)] * 2
    if not forward:
        shapes.append(jax.ShapeDtypeStruct((8, width), F32))
        if not last:
            shapes.append(jax.ShapeDtypeStruct((rows_own, width), F32))
    if bulk is not None:
        more = tuple(more) + (bulk,)
        piece = bulk.shape[-3:]
        shapes.append(jax.ShapeDtypeStruct(((lax.axis_size("dp"),) if forward else ()) + piece, BF16))
        if mode == "backward_last":
            shapes.append(jax.ShapeDtypeStruct(piece, BF16))
    moved = full_width if forward else width
    siblings = cores - 1
    sem = pltpu.SemaphoreType.DMA
    scratch = [
        pltpu.VMEM((cores, 2, rows_own, moved), BF16),
        pltpu.VMEM((siblings, 2, rows_own, moved), BF16),
        pltpu.VMEM((2, rows_own, moved), BF16),
        pltpu.VMEM((2, rows_own, moved), BF16),
    ]
    if last:
        scratch.append(pltpu.VMEM((rows_own, width), BF16 if forward else F32))
    if bulk is not None and not forward:
        scratch.append(pltpu.VMEM((seqs, 2) + piece[1:], BF16))
        scratch.append(pltpu.VMEM(piece, BF16))
    scratch += [
        sem((siblings, 2)), sem((siblings, 2)), sem((2, chunks)), sem((2, chunks)),
        sem((2, chunks)), sem((2, chunks)), sem((siblings, 2, chunks)), sem((siblings, 2, chunks)),
        sem((chunks,)), sem((max(share // chunk, 1),)),
    ]
    if bulk is not None:
        scratch += [sem((seqs, 2)), sem((seqs, 2)), sem((seqs,)), sem((seqs,))]
    if mode == "backward_last":
        scratch += [sem((seqs - 1,)), sem((seqs - 1,))]
    return pl.pallas_call(
        functools.partial(reduce_kernel, mode, dims),
        out_shape=shapes,
        in_specs=[VMEM_SPEC] * (3 + len(more)),
        out_specs=[VMEM_SPEC] * len(shapes),
        scratch_shapes=scratch,
        compiler_params=pltpu.CompilerParams(
            vmem_limit_bytes=60 * 1024 * 1024, collective_id=ident, has_side_effects=True
        ),
        name=mode,
    )(lhs, rhs, gain, *more)


def begin_kernel(dims, pack_ref, rows_ref, pack_out, rows_out, *sems):
    seqs, cores, share, chunk = dims
    ex_ss, ex_rs, near_ss, near_rs, far_ss, far_rs, ag_ss, ag_rs, sib_ss, sib_rs, here = sems
    place, core, part = (lax.axis_index(a) for a in ("seq", "tensor", "dp"))
    mesh_id = pl.DeviceIdType.MESH
    near = {1: part + 1 - 2 * lax.rem(part, 2), 2: lax.rem(part + 2, 4)}
    barrier = pltpu.get_barrier_semaphore()
    peers = [{"dp": near[1]}, {"dp": near[2]}]
    for a in range(seqs):
        for b in range(cores):
            if a or b:
                peers.append(
                    {"seq": lax.rem(place + a, seqs), "tensor": lax.rem(core + b, cores)}
                )
    for peer in peers:
        pl.semaphore_signal(barrier, inc=1, device_id=peer, device_id_type=mesh_id)
    pl.semaphore_wait(barrier, len(peers))

    def remote(source, target, send_sem, recv_sem, device):
        return pltpu.make_async_remote_copy(
            src_ref=source, dst_ref=target, send_sem=send_sem, recv_sem=recv_sem,
            device_id=device, device_id_type=mesh_id,
        )

    def exchange(o):
        to = lax.rem(place + o, seqs)
        return remote(
            pack_ref.at[to], pack_out.at[part, place], ex_ss.at[o - 1], ex_rs.at[o - 1],
            {"seq": to},
        )

    def arrive(o):
        return lax.rem(place - o + seqs, seqs)

    def to_near(o, bit):
        target = pack_out.at[part, arrive(o)]
        return remote(
            target, target, near_ss.at[o, bit - 1], near_rs.at[o, bit - 1],
            {"dp": near[bit]},
        )

    def to_far(o):
        bit = 1 + o % 2
        target = pack_out.at[near[bit], arrive(o)]
        return remote(
            target, target, far_ss.at[o], far_rs.at[o], {"dp": near[3 - bit]}
        )

    def block_rows(at_place, at_core, k):
        start = (at_place * cores + at_core) * share + k * chunk
        return pl.ds(pl.multiple_of(start, chunk), chunk)

    def along(direction, d, k):
        target = rows_out.at[block_rows(place - direction * d, core, k)]
        at = (direction + 1) // 2
        return remote(
            target, target, ag_ss.at[at, d, k], ag_rs.at[at, d, k], {"seq": place + direction}
        )

    def beside(direction, d, k, o, at_core):
        target = rows_out.at[block_rows(place - direction * d, at_core, k)]
        at = (direction + 1) // 2
        return remote(
            target, target, sib_ss.at[at, d, k, o - 1], sib_rs.at[at, d, k, o - 1],
            {"tensor": lax.rem(core + o, cores)},
        )

    chunks = share // chunk
    for o in range(1, seqs):
        exchange(o).start()
    own = [
        pltpu.make_async_copy(rows_ref, rows_out.at[block_rows_all(place, core, cores, share)], here.at[0])
    ]
    own.append(pltpu.make_async_copy(pack_ref.at[place], pack_out.at[part, place], here.at[1]))
    for copy in own:
        copy.start()
    for copy in own:
        copy.wait()

    def can(direction):
        return place < seqs - 1 if direction > 0 else place > 0

    def exists(direction, d):
        return place - d >= 0 if direction > 0 else place + d < seqs

    for k in range(chunks):
        for direction in (1, -1):

            @pl.when(can(direction))
            def _():
                along(direction, 0, k).start()

        for o in range(1, cores):
            beside(1, 0, k, o, core).start()
    for bit in (1, 2):
        to_near(0, bit).start()
    for o in range(1, seqs):
        exchange(o).wait_recv()
        for bit in (1, 2):
            to_near(o, bit).start()
    def rows_from(d):
        def pass_on(k, carry):
            for direction in (1, -1):

                @pl.when(exists(direction, d))
                def _():
                    along_in(along, direction, d, k)

                    @pl.when(can(direction))
                    def _():
                        along(direction, d, k).start()

                    for o in range(1, cores):
                        beside(direction, d, k, o, core).start()

            return carry

        lax.fori_loop(0, chunks, pass_on, 0)

    def far(o):
        for bit in (1, 2):
            to_near(o, bit).wait_recv()
        to_far(o).start()

    far(0)
    far(1)
    rows_from(1)
    for o in range(2, seqs):
        far(o)
        rows_from(o)
    for o in range(seqs):
        to_far(o).wait()
        for bit in (1, 2):
            to_near(o, bit).wait_send()
        if o:
            exchange(o).wait_send()

    def drain(k, carry):
        for d in range(seqs):
            for direction in (1, -1):

                @pl.when(jnp.logical_and(exists(direction, d), can(direction)))
                def _():
                    along(direction, d, k).wait_send()

                if d > 0 or direction > 0:

                    @pl.when(exists(direction, d))
                    def _():
                        for o in range(1, cores):
                            beside(direction, d, k, o, core).wait_send()
                            beside(direction, d, k, o, lax.rem(core - o + cores, cores)).wait_recv()

        return carry

    lax.fori_loop(0, chunks, drain, 0)


def block_rows_all(place, core, cores, share):
    return pl.ds(pl.multiple_of((place * cores + core) * share, share), share)


def along_in(along, direction, d, k):
    along(direction, d - 1, k).wait_recv()


def run_begin(ident, pack, rows, parts):
    seqs, cores = lax.axis_size("seq"), lax.axis_size("tensor")
    share, width = rows.shape
    chunk = min(64, share)
    chunks = share // chunk
    sem = pltpu.SemaphoreType.DMA
    return pl.pallas_call(
        functools.partial(begin_kernel, (seqs, cores, share, chunk)),
        out_shape=(
            jax.ShapeDtypeStruct((parts,) + pack.shape, BF16),
            jax.ShapeDtypeStruct((seqs * cores * share, width), BF16),
        ),
        in_specs=[VMEM_SPEC] * 2,
        out_specs=[VMEM_SPEC] * 2,
        scratch_shapes=[
            sem((seqs - 1,)), sem((seqs - 1,)), sem((seqs, 2)), sem((seqs, 2)),
            sem((seqs,)), sem((seqs,)), sem((2, seqs, chunks)), sem((2, seqs, chunks)),
            sem((2, seqs, chunks, cores - 1)), sem((2, seqs, chunks, cores - 1)), sem((2,)),
        ],
        compiler_params=pltpu.CompilerParams(
            vmem_limit_bytes=56 * 1024 * 1024, collective_id=ident, has_side_effects=True
        ),
        name="begin",
    )(pack, rows)


def conv_silu(padded, kernel):
    row_count = padded.shape[0] - K + 1
    running = kernel[K]
    for offset in range(K):
        running = running + kernel[offset] * padded[offset : offset + row_count]
    return jax.nn.silu(running)


def prenorm(residual, gain_pre):
    return (
        residual
        * lax.rsqrt(jnp.mean(residual * residual, axis=-1, keepdims=True) + EPSILON)
        * gain_pre
    )


def pad_to(value, rows, columns):
    return jnp.pad(value, ((0, rows - value.shape[0]), (0, columns - value.shape[1])))


def body(
    hidden, lengths, pre_gain, w_zx, w_bc, w_dt, conv_x, conv_bc, head_params,
    norm_gain, w_out, cotangent,
):
    seqs, cores, parts = (lax.axis_size(a) for a in ("seq", "tensor", "dp"))
    place, core = lax.axis_index("seq"), lax.axis_index("tensor")
    piece, width = hidden.shape[1], hidden.shape[2]
    tokens, share = piece * seqs, piece // cores
    depth = w_zx.shape[1]
    inner = w_zx.shape[3] // seqs
    heads = w_dt.shape[2] // seqs
    pair_cols = w_bc.shape[2]
    bc_at = 2 * inner
    step_at = bc_at + -(-pair_cols // LANES) * LANES
    sizes = (tokens, inner, heads, step_at)
    live = (jnp.arange(tokens, dtype=jnp.int32) < lengths[0]).astype(F32)[:, None]

    def own_rows(value):
        return lax.dynamic_slice_in_dim(value[0], core * share, share, 0)

    def packed(layer, w_zx, w_bc, w_dt, w_out):
        mix = w_out[layer].reshape(seqs, inner, depth).transpose(0, 2, 1)
        wide = [
            w_zx[layer][:, g].reshape(depth, seqs, inner).transpose(1, 0, 2) for g in (0, 1)
        ]
        pair_part = jnp.broadcast_to(w_bc[layer][None], (seqs, depth, pair_cols))
        pair_part = jnp.pad(pair_part, ((0, 0), (0, 0), (0, step_at - bc_at - pair_cols)))
        step_part = w_dt[layer].reshape(depth, seqs, heads).transpose(1, 0, 2)
        step_part = jnp.pad(step_part, ((0, 0), (0, 0), (0, LANES - heads)))
        return jnp.concatenate([mix] + wide + [pair_part, step_part], axis=2)

    pack, hidden_full = run_begin(
        2 * L, packed(0, w_zx, w_bc, w_dt, w_out), own_rows(hidden), parts
    )
    weights = [pack.reshape(width, -1)]
    w_zx, w_bc, w_dt, w_out, hidden_full = lax.optimization_barrier(
        (w_zx, w_bc, w_dt, w_out, hidden_full)
    )
    coming = exchange_axis(packed(1, w_zx, w_bc, w_dt, w_out), "seq")

    def end_rows(value):
        upper = place >= seqs // 2
        shaped = value.reshape(2, seqs // 2, cores, share, width)
        mine = pick(jnp.moveaxis(pick(shaped, upper.astype(jnp.int32)), 1, 0), core)
        return jnp.where(upper, mine, mine[::-1]).reshape(seqs // 2 * share, width)

    residual = end_rows(hidden_full).astype(F32)
    normed = prenorm(hidden_full.astype(F32), pre_gain[0]).astype(BF16)

    def tensor_columns(value):
        if cores == 2:
            other = swap(value, "tensor", 1)
            first = jnp.where(core == 0, value, other)
            return jnp.concatenate([first, jnp.where(core == 0, other, value)], axis=1)
        parts_of = gather_axis(value, "tensor")
        return jnp.moveaxis(parts_of, 0, 1).reshape(value.shape[0], -1)

    kept = []
    for layer in range(L):
        conv = pad_to(
            lax.dynamic_slice_in_dim(conv_x[layer], place * inner, inner, 1), 8, inner
        )
        head_rows = pad_to(
            lax.dynamic_slice_in_dim(head_params[layer], place * heads, heads, 1), 8, LANES
        )
        gain = lax.dynamic_slice_in_dim(norm_gain[layer], place * inner, inner, 0)[None]
        entry = residual
        proj = jnp.dot(normed, weights[layer][:, inner:], preferred_element_type=F32)
        pair_raw = (proj[:, bc_at : bc_at + pair_cols] * live).astype(BF16)
        padded_pair = jnp.pad(pair_raw.astype(F32), ((K - 1, 0), (0, 0)))
        pairs = tensor_columns(conv_silu(padded_pair, conv_bc[layer]).astype(BF16))
        outputs, mixed, inputs, states, squares = run_forward(
            sizes, lengths, proj, pairs, conv, head_rows, gain
        )
        if layer + 1 < L:
            full, residual, raw, pack = run_reduce(
                "forward_middle", layer, mixed, weights[layer], pre_gain[layer + 1][None],
                (squares, residual), coming,
            )
            weights.append(pack.reshape(width, -1))
            extra = full[:, width:]
            cotangent, full = lax.optimization_barrier((cotangent, full))
            upstream_full = gather_rows(own_rows(cotangent))
            upstream = end_rows(upstream_full)
        else:
            extra, result_low = run_reduce(
                "forward_last", layer, mixed, weights[layer], pre_gain[layer][None],
                (squares, residual, upstream),
            )
            raw, up_extra = None, extra
        kept.append(
            (entry, raw, normed, proj, padded_pair, pairs, outputs, inputs, states, extra,
             conv, head_rows, gain)
        )
        if layer + 1 < L:
            normed = full[:, :width]

    shared, owned, pair_convs = [None] * L, [None] * L, [None] * L
    weight_grads = [None] * L
    for layer in reversed(range(L)):
        (entry, raw, normed, proj, padded_pair, pairs, outputs, inputs, states, extra,
         conv, head_rows, gain) = kept[layer]
        mixed_in, slab, bc, conv_grad, head_grad, small = run_backward(
            sizes, lengths, proj, pairs, conv, head_rows, gain, inputs, outputs, states,
            upstream_full, weights[layer], extra, up_extra,
        )
        bc = jnp.moveaxis(bc.reshape(tokens, cores, pair_cols), 1, 0)
        bc = sum_axis(scatter_axis(bc, "tensor", F32), "seq", BF16)
        unused, pull_pair = jax.vjp(conv_silu, padded_pair, conv_bc[layer])
        d_padded, d_conv_bc = pull_pair(bc)
        d_pair = (d_padded[K - 1 :] * live).astype(BF16)
        slab = lax.dynamic_update_slice_in_dim(
            slab, pad_to(d_pair / seqs, tokens, step_at - bc_at), bc_at, 1
        )
        grads = jnp.concatenate(
            [
                lax.dot_general(
                    upstream_full[:, :width], mixed_in, (TN, ((), ())), preferred_element_type=F32
                ).astype(BF16),
                lax.dot_general(
                    normed, slab, (TN, ((), ())), preferred_element_type=F32
                ).astype(BF16),
            ],
            axis=1,
        ).reshape(parts, seqs, depth, -1)
        if layer > 0:
            upstream_full, d_pre, upstream, grads = run_reduce(
                "backward_middle", L + layer, slab, weights[layer], pre_gain[layer][None],
                (entry, upstream, kept[layer - 1][1]), grads,
            )
            up_extra = upstream_full[:, width:]
            weight_grads[layer] = exchange_axis(grads, "seq")
        else:
            d_own, d_pre, grads, weight_grads[layer] = run_reduce(
                "backward_last", L + layer, slab, weights[layer], pre_gain[layer][None],
                (entry, upstream), grads,
            )
        skip = small[1].reshape(heads, P_SIZE).sum(-1)
        shared[layer] = d_pre[0]
        pair_convs[layer] = d_conv_bc
        owned[layer] = jnp.concatenate(
            [conv_grad[: K + 1].reshape(-1), small[0], head_grad[:2, :heads].reshape(-1), skip]
        )

    result = gather_axis(result_low, "tensor").reshape(piece, width)
    d_hidden = gather_axis(d_own, "tensor").reshape(piece, width)
    d_pre = jnp.stack(shared)
    for axis in ("dp", "seq", "tensor"):
        d_pre = sum_axis(d_pre, axis)
    small_sums = sum_axis(jnp.stack(owned), "dp")
    small_all = jnp.moveaxis(gather_axis(small_sums, "seq"), 0, 1)
    pair_sums = sum_axis(jnp.stack(pair_convs), "dp")

    def columns(first, count, each):
        part = small_all[:, :, first : first + count * each].reshape(L, seqs, count, each)
        return part.transpose(0, 2, 1, 3).reshape(L, count, seqs * each)

    edge = (K + 1) * inner
    all_grads = jnp.stack(weight_grads).astype(F32)
    d_zx = [
        all_grads[..., g * inner : (g + 1) * inner].transpose(0, 2, 1, 3).reshape(L, depth, -1)
        for g in (1, 2)
    ]
    d_mix = all_grads[..., :inner].transpose(0, 1, 3, 2).reshape(L, seqs * inner, depth)
    bc_at, step_at = inner + bc_at, inner + step_at
    d_bc = all_grads[..., bc_at : bc_at + pair_cols].sum(1)
    d_dt = all_grads[..., step_at : step_at + heads].transpose(0, 2, 1, 3)
    return (
        result[None],
        d_hidden[None],
        d_pre,
        jnp.stack(d_zx, axis=2),
        d_bc,
        d_dt.reshape(L, depth, seqs * heads),
        columns(0, K + 1, inner),
        pair_sums,
        columns(edge + inner, 3, heads),
        columns(edge, 1, inner)[:, 0],
        d_mix,
    )


def solution(mesh):
    wide = P(None, ("dp", "seq"), None, "tensor")
    thin = P(None, ("dp", "seq"), "tensor")
    rows = P("dp", "seq", None)
    flat = P(None, None, "tensor")
    gain = P(None, "tensor")
    mix = P(None, "tensor", ("dp", "seq"))
    return jax.shard_map(
        body,
        mesh=mesh,
        in_specs=(rows, P("dp"), P(), wide, thin, thin, flat, flat, flat, gain, mix, rows),
        out_specs=(rows, rows, P(), wide, thin, thin, flat, flat, flat, gain, mix),
        check_vma=False,
    )
```
